32 devices in a mesh: frag: 2 (over x), dev: 16 (over z, y, core).
Axes of the slice: x: 2, y: 2, z: 4, core: 2. Of those that a mesh axis runs over, the one named last changes fastest.
Arguments:
- ao_ints: bfloat16 [192, 96, 96, 96], P(('frag', 'dev')), parts along dimension 0
- coeffs: bfloat16 [192, 96], P('frag'), parts along dimension 0
Outputs:
- output: float32 [192, 96, 9216], P('frag', None, 'dev'), parts along dimension 0
There are 2 independent parts. The reference program is written for one: setup_inputs(seed, part) draws one part's arguments, and reference() takes and returns one part's arrays. A program takes and returns all parts, laid end to end along the dimension named above; each array names one.
All inputs are finite; a program needn't handle non-finite values.
Results may differ from the reference program's by a relative error of at most 0.001.
Values are sent between devices in bfloat16 or wider.
A program may use at most 1 GiB of HBM per device.

```python
import jax
import jax.numpy as jnp
from jax import lax

NBASIS = 96


def setup_inputs(seed: int = 0, part: int = 0) -> dict:
    part_key = jax.random.fold_in(jax.random.key(seed), part)
    key_ints, key_coef = jax.random.split(part_key)
    ao_ints = jax.random.normal(key_ints, (NBASIS, NBASIS, NBASIS, NBASIS), jnp.float32).astype(jnp.bfloat16)
    coeffs = (jax.random.normal(key_coef, (NBASIS, NBASIS), jnp.float32) * NBASIS ** -0.5).astype(jnp.bfloat16)
    return {"ao_ints": ao_ints, "coeffs": coeffs}


def reference(ao_ints, coeffs):
    n_basis = coeffs.shape[0]
    coeffs_t = coeffs.T

    def row_transform(a_row):
        a_qsr = jnp.transpose(a_row, (0, 2, 1)).reshape(n_basis * n_basis, n_basis)
        t_one = jnp.dot(a_qsr, coeffs, preferred_element_type=jnp.float32).astype(jnp.bfloat16)
        t_qjs = jnp.transpose(t_one.reshape(n_basis, n_basis, n_basis), (0, 2, 1)).reshape(n_basis * n_basis, n_basis)
        h_row = jnp.dot(t_qjs, coeffs, preferred_element_type=jnp.float32).astype(jnp.bfloat16)
        return jnp.dot(coeffs_t, h_row.reshape(n_basis, n_basis * n_basis), preferred_element_type=jnp.float32).astype(jnp.bfloat16)

    g_all = lax.map(row_transform, ao_ints)
    mo_ints = jnp.dot(coeffs_t, g_all.reshape(n_basis, n_basis ** 3), preferred_element_type=jnp.float32)
    return mo_ints.reshape(n_basis, n_basis, n_basis * n_basis)
```

```python
import functools

import jax
import jax.numpy as jnp
from jax import lax
from jax.experimental import pallas as pl
from jax.experimental.pallas import tpu as pltpu
from jax.sharding import PartitionSpec as P

MESH = pl.DeviceIdType.MESH
N = 96
DEV = 16
PAIRS = 3
COLS = 6
QPAD = 104
QB = 8
TILES = 54


def iota(shape, dim):
    return lax.broadcasted_iota(jnp.int32, shape, dim)


def onehot(mask):
    return jnp.where(mask, 1.0, 0.0).astype(jnp.bfloat16)


def dot(x, y, dims=((1,), (0,))):
    return lax.dot_general(x, y, (dims, ((), ())), preferred_element_type=jnp.float32)


def exchange_kernel(a_hbm, c_ref, g_hbm, kc_ref, a_vm, h_scr, send, cc_ref, a_sem, send_sem, recv_sem, own_sem):
    frag = lax.axis_index('frag')
    me = lax.axis_index('dev')
    chip, core = me // 2, me % 2
    cz1, cz0, cy = chip // 4, (chip // 2) % 2, chip % 2

    def load(p, part):
        quarter = pl.ds(part * (N // 4), N // 4)
        return pltpu.make_async_copy(a_hbm.at[p, quarter], a_vm.at[p, quarter], a_sem.at[p, part])

    for p in range(2 * PAIRS):
        for part in range(4):
            load(p, part).start()

    barrier = pltpu.get_barrier_semaphore()

    @pl.loop(1, DEV)
    def _(k):
        pl.semaphore_signal(barrier, inc=1, device_id=(frag, (me + k) % DEV), device_id_type=MESH)

    c = c_ref[...]
    eye = onehot(iota((N, N), 0) == iota((N, N), 1))
    ct = dot(eye, c, ((1,), (1,))).astype(jnp.bfloat16)
    c_pad = dot(c, onehot(iota((N, 128), 0) == iota((N, 128), 1))).astype(jnp.bfloat16)
    row = iota((2 * N, N), 0)
    pick_a = onehot(iota((2 * N, N), 1) == 8 * (row // 16) + row % 8)
    c_rows = dot(pick_a, c, ((1,), (1,))).astype(jnp.bfloat16)
    wide = dot(c_rows, onehot(iota((N, 2 * N), 1) % N == iota((N, 2 * N), 0)))
    same_p = (iota((2 * N, 2 * N), 0) % 16) // 8 == iota((2 * N, 2 * N), 1) // N
    cc_ref[...] = jnp.where(same_p, wide, 0.0).astype(jnp.bfloat16)

    pl.semaphore_wait(barrier, DEV - 1)

    lane = iota((N, 128), 1)

    def copy_out(pp, dest):
        return pltpu.make_async_remote_copy(
            src_ref=send.at[pp, dest],
            dst_ref=g_hbm.at[me * PAIRS + pp],
            send_sem=send_sem.at[pp, dest],
            recv_sem=recv_sem.at[pp, me],
            device_id=(frag, dest),
            device_id_type=MESH,
        )

    def copy_own(pp):
        return pltpu.make_async_copy(send.at[pp, me], g_hbm.at[me * PAIRS + pp], own_sem.at[pp])

    def pack(pp, dest_chip):
        halves = []
        for p in range(2):
            tiles, last = [], []
            for cc in range(2):
                j0 = (dest_chip * 2 + cc) * COLS
                x = [h_scr[p, pl.ds(pl.multiple_of((j0 + l) * QPAD, 8), N), :] for l in range(COLS)]
                r1, r2, r3 = pltpu.roll(x[1], 96, 1), pltpu.roll(x[2], 64, 1), pltpu.roll(x[3], 32, 1)
                r5 = pltpu.roll(x[5], 96, 1)
                tiles += [jnp.where(lane < 96, x[0], r1), jnp.where(lane < 64, r1, r2),
                          jnp.where(lane < 32, r2, r3), jnp.where(lane < 96, x[4], r5)]
                last.append(r5 if cc == 0 else pltpu.roll(x[5], 32, 1))
            tiles.append(jnp.where(lane < 64, last[0], last[1]))
            halves.append(jnp.concatenate([t.astype(jnp.bfloat16) for t in tiles], axis=1))
        rhs = jnp.concatenate(halves, axis=0)
        out = dot(cc_ref[...], rhs)
        for cc in range(2):
            dest = dest_chip * 2 + cc
            for t in range(4):
                tile = out[:, (cc * 4 + t) * 128:(cc * 4 + t + 1) * 128].astype(jnp.bfloat16)
                for g in range(12):
                    send[pp, dest, g * 4 + t] = tile[g * 16:(g + 1) * 16]
        low = iota((16, 128), 1) < 64
        for u in range(6):
            upper = out[u * 32:u * 32 + 16, 1024:]
            lower = out[u * 32 + 16:u * 32 + 32, 1024:]
            send[pp, dest_chip * 2, 48 + u] = jnp.where(low, upper, pltpu.roll(lower, 64, 1)).astype(jnp.bfloat16)
            send[pp, dest_chip * 2 + 1, 48 + u] = jnp.where(low, pltpu.roll(upper, 64, 1), lower).astype(jnp.bfloat16)

    @pl.loop(0, PAIRS)
    def _(pp):
        for p2 in range(2):
            p = pp * 2 + p2
            for part in range(4):
                load(p, part).wait()

                @pl.loop(0, N // 4 // QB)
                def _(qb):
                    q0 = part * (N // 4) + qb * QB
                    t_rows = [dot(ct, a_vm[p, q0 + i]).astype(jnp.bfloat16) for i in range(QB)]
                    half = dot(jnp.concatenate(t_rows, axis=0), c_pad)
                    for i in range(QB):
                        h_scr[p2, pl.ds(q0 + i, N, stride=QPAD), :] = half[i * N:(i + 1) * N]

        @pl.loop(0, 7)
        def _(t):
            m = 7 - t
            dest_chip = 4 * ((cz1 + m // 4) % 2) + 2 * ((cz0 + (m // 2) % 2) % 2) + (cy + m % 2) % 2
            pack(pp, dest_chip)
            copy_out(pp, dest_chip * 2).start()
            copy_out(pp, dest_chip * 2 + 1).start()

        pack(pp, chip)
        copy_out(pp, chip * 2 + 1 - core).start()
        copy_own(pp).start()

    m8 = 8 * N
    spread = dot(onehot(iota((m8, N), 0) // 8 == iota((m8, N), 1)), c, ((1,), (1,))).astype(jnp.bfloat16)
    full = dot(spread, onehot(iota((N, m8), 1) // 8 == iota((N, m8), 0)))
    same = iota((m8, m8), 0) % 8 == iota((m8, m8), 1) % 8
    kc_ref[...] = jnp.where(same, full, 0.0).astype(jnp.bfloat16)

    @pl.loop(0, PAIRS)
    def _(pp):
        copy_own(pp).wait()

        @pl.loop(1, DEV)
        def _(k):
            copy_out(pp, (me + k) % DEV).wait_send()

        @pl.loop(1, DEV)
        def _(k):
            src = (me + k) % DEV
            pltpu.make_async_remote_copy(
                src_ref=send.at[pp, src], dst_ref=g_hbm.at[src * PAIRS + pp],
                send_sem=send_sem.at[pp, src], recv_sem=recv_sem.at[pp, src],
                device_id=(frag, src), device_id_type=MESH,
            ).wait_recv()


def last_kernel(main_ref, half_ref, kc_ref, v_ref):
    kc = kc_ref[...]
    k = 8 * N
    for gg in range(2):
        for n in range(2):
            rhs = jnp.concatenate([main_ref[:, gg * 4 + 2 * n + t].reshape(k, 128) for t in range(2)], axis=1)
            out = dot(kc, rhs)
            v_ref[:, gg * 8:(gg + 1) * 8, n * 256:(n + 1) * 256] = out.reshape(N, 8, 256)
    out = dot(kc, half_ref[:, 0].reshape(k, 128))
    v_ref[:, 0:8, 512:576] = out.reshape(N, 8, 128)[:, :, :64]
    v_ref[:, 8:16, 512:576] = pltpu.roll(out, 64, 1).reshape(N, 8, 128)[:, :, :64]


def solution(mesh):
    def local_transform(ao_rows, coeffs):
        blocks = DEV * PAIRS
        g_all, kc = pl.pallas_call(
            exchange_kernel,
            out_shape=(jax.ShapeDtypeStruct((blocks, TILES, 16, 128), jnp.bfloat16),
                       jax.ShapeDtypeStruct((8 * N, 8 * N), jnp.bfloat16)),
            in_specs=[pl.BlockSpec(memory_space=pltpu.HBM), pl.BlockSpec(memory_space=pltpu.VMEM)],
            out_specs=(pl.BlockSpec(memory_space=pltpu.HBM), pl.BlockSpec(memory_space=pltpu.VMEM)),
            scratch_shapes=[
                pltpu.VMEM((2 * PAIRS, N, N, N), jnp.bfloat16),
                pltpu.VMEM((2, N * QPAD, 128), jnp.float32),
                pltpu.VMEM((PAIRS, DEV, TILES, 16, 128), jnp.bfloat16),
                pltpu.VMEM((2 * N, 2 * N), jnp.bfloat16),
                pltpu.SemaphoreType.DMA((2 * PAIRS, 4)),
                pltpu.SemaphoreType.DMA((PAIRS, DEV)),
                pltpu.SemaphoreType.DMA((PAIRS, DEV)),
                pltpu.SemaphoreType.DMA((PAIRS,)),
            ],
            compiler_params=pltpu.CompilerParams(collective_id=0, has_side_effects=True, vmem_limit_bytes=60 * 2**20),
            cost_estimate=pl.CostEstimate(flops=6 * 10**9, bytes_accessed=40 * 10**6, transcendentals=0),
            name='exchange',
        )(ao_rows, coeffs)
        return pl.pallas_call(
            last_kernel,
            grid=(6,),
            out_shape=jax.ShapeDtypeStruct((N, N, COLS * N), jnp.float32),
            in_specs=[
                pl.BlockSpec((blocks, 8, 16, 128), lambda u: (0, u, 0, 0)),
                pl.BlockSpec((blocks, 1, 16, 128), lambda u: (0, 48 + u, 0, 0)),
                pl.BlockSpec((8 * N, 8 * N), lambda u: (0, 0)),
            ],
            out_specs=pl.BlockSpec((N, 16, COLS * N), lambda u: (0, u, 0)),
            compiler_params=pltpu.CompilerParams(vmem_limit_bytes=48 * 2**20),
            cost_estimate=pl.CostEstimate(flops=8 * 10**9, bytes_accessed=35 * 10**6, transcendentals=0),
            name='last_product',
        )(g_all, g_all, kc)

    return jax.shard_map(local_transform, mesh=mesh, in_specs=(P(('frag', 'dev')), P('frag')), out_specs=P('frag', None, 'dev'), check_vma=False)
```

```python
import functools

import jax
import jax.numpy as jnp
from jax import lax
from jax.experimental import pallas as pl
from jax.experimental.pallas import tpu as pltpu
from jax.sharding import PartitionSpec as P

MESH = pl.DeviceIdType.MESH
N = 96
DEV = 16
PAIRS = 3
COLS = 6
QPAD = 104
QB = 8
TILES = 54


def iota(shape, dim):
    return lax.broadcasted_iota(jnp.int32, shape, dim)


def onehot(mask):
    return jnp.where(mask, 1.0, 0.0).astype(jnp.bfloat16)


def dot(x, y, dims=((1,), (0,))):
    return lax.dot_general(x, y, (dims, ((), ())), preferred_element_type=jnp.float32)


def exchange_kernel(a_hbm, c_hbm, g_hbm, kc_ref, a_vm, c_vm, h_scr, send, cc_ref, a_sem, c_sem, send_sem, recv_sem, own_sem):
    frag = lax.axis_index('frag')
    me = lax.axis_index('dev')
    chip, core = me // 2, me % 2
    cz1, cz0, cy = chip // 4, (chip // 2) % 2, chip % 2
    edge = 1 - (cz1 + cz0) % 2

    def load(p, part):
        quarter = pl.ds(part * (N // 4), N // 4)
        return pltpu.make_async_copy(a_hbm.at[p, quarter], a_vm.at[p, quarter], a_sem.at[p, part])

    load_c = pltpu.make_async_copy(c_hbm, c_vm, c_sem)
    load_c.start()
    for p in range(2 * PAIRS):
        for part in range(4):
            load(p, part).start()

    barrier = pltpu.get_barrier_semaphore()

    @pl.loop(1, DEV)
    def _(k):
        pl.semaphore_signal(barrier, inc=1, device_id=(frag, (me + k) % DEV), device_id_type=MESH)

    load_c.wait()
    c = c_vm[...]
    eye = onehot(iota((N, N), 0) == iota((N, N), 1))
    ct = dot(eye, c, ((1,), (1,))).astype(jnp.bfloat16)
    r2, c2 = iota((256, N), 0), iota((N, 256), 1)
    stacked = dot(onehot(r2 % 128 == iota((256, N), 1)), c).astype(jnp.bfloat16)
    both = dot(stacked, onehot(c2 % 128 == iota((N, 256), 0)))
    c_two = jnp.where(iota((256, 256), 0) // 128 == iota((256, 256), 1) // 128, both, 0.0).astype(jnp.bfloat16)
    gap = jnp.zeros((N, 32), jnp.bfloat16)
    row = iota((2 * N, N), 0)
    pick_a = onehot(iota((2 * N, N), 1) == 8 * (row // 16) + row % 8)
    c_rows = dot(pick_a, c, ((1,), (1,))).astype(jnp.bfloat16)
    wide = dot(c_rows, onehot(iota((N, 2 * N), 1) % N == iota((N, 2 * N), 0)))
    same_p = (iota((2 * N, 2 * N), 0) % 16) // 8 == iota((2 * N, 2 * N), 1) // N
    cc_ref[...] = jnp.where(same_p, wide, 0.0).astype(jnp.bfloat16)

    pl.semaphore_wait(barrier, DEV - 1)

    lane = iota((N, 128), 1)

    def copy_out(pp, dest):
        return pltpu.make_async_remote_copy(
            src_ref=send.at[pp, dest],
            dst_ref=g_hbm.at[me * PAIRS + pp],
            send_sem=send_sem.at[pp, dest],
            recv_sem=recv_sem.at[pp, me],
            device_id=(frag, dest),
            device_id_type=MESH,
        )

    def copy_own(pp):
        return pltpu.make_async_copy(send.at[pp, me], g_hbm.at[me * PAIRS + pp], own_sem.at[pp])

    def pack(pp, dest_chip):
        halves = []
        for p in range(2):
            tiles, last = [], []
            for cc in range(2):
                j0 = (dest_chip * 2 + cc) * COLS
                x = [h_scr[p, pl.ds(pl.multiple_of((j0 + l) * QPAD, 8), N), :] for l in range(COLS)]
                r1, r2, r3 = pltpu.roll(x[1], 96, 1), pltpu.roll(x[2], 64, 1), pltpu.roll(x[3], 32, 1)
                r5 = pltpu.roll(x[5], 96, 1)
                tiles += [jnp.where(lane < 96, x[0], r1), jnp.where(lane < 64, r1, r2),
                          jnp.where(lane < 32, r2, r3), jnp.where(lane < 96, x[4], r5)]
                last.append(r5 if cc == 0 else pltpu.roll(x[5], 32, 1))
            tiles.append(jnp.where(lane < 64, last[0], last[1]))
            halves.append(jnp.concatenate([t.astype(jnp.bfloat16) for t in tiles], axis=1))
        rhs = jnp.concatenate(halves, axis=0)
        out = dot(cc_ref[...], rhs)
        for cc in range(2):
            dest = dest_chip * 2 + cc
            for t in range(4):
                tile = out[:, (cc * 4 + t) * 128:(cc * 4 + t + 1) * 128].astype(jnp.bfloat16)
                for g in range(12):
                    send[pp, dest, g * 4 + t] = tile[g * 16:(g + 1) * 16]
        low = iota((16, 128), 1) < 64
        for u in range(6):
            upper = out[u * 32:u * 32 + 16, 1024:]
            lower = out[u * 32 + 16:u * 32 + 32, 1024:]
            send[pp, dest_chip * 2, 48 + u] = jnp.where(low, upper, pltpu.roll(lower, 64, 1)).astype(jnp.bfloat16)
            send[pp, dest_chip * 2 + 1, 48 + u] = jnp.where(low, pltpu.roll(upper, 64, 1), lower).astype(jnp.bfloat16)

    @pl.loop(0, PAIRS)
    def _(pp):
        for p2 in range(2):
            p = pp * 2 + p2
            for part in range(4):
                load(p, part).wait()

                @pl.loop(0, N // 4 // QB)
                def _(qb):
                    q0 = part * (N // 4) + qb * QB
                    t_rows = []
                    for i in range(0, QB, 2):
                        two = jnp.concatenate([a_vm[p, q0 + i], gap, a_vm[p, q0 + i + 1], gap], axis=1)
                        t_rows.append(dot(ct, two).astype(jnp.bfloat16))
                    half = dot(jnp.concatenate(t_rows, axis=0), c_two)
                    for i in range(QB):
                        rows = half[(i // 2) * N:(i // 2 + 1) * N, (i % 2) * 128:(i % 2 + 1) * 128]
                        h_scr[p2, pl.ds(q0 + i, N, stride=QPAD), :] = rows

        @pl.loop(0, 8)
        def _(t):
            m = (7 - t + 4 * edge) % 8
            dest_chip = 4 * ((cz1 + m // 4) % 2) + 2 * ((cz0 + (m // 2) % 2) % 2) + (cy + m % 2) % 2
            pack(pp, dest_chip)
            for cc in range(2):
                dest = dest_chip * 2 + cc

                @pl.when(dest != me)
                def _():
                    copy_out(pp, dest).start()

                @pl.when(dest == me)
                def _():
                    copy_own(pp).start()

    m8 = 8 * N
    spread = dot(onehot(iota((m8, N), 0) // 8 == iota((m8, N), 1)), c, ((1,), (1,))).astype(jnp.bfloat16)
    full = dot(spread, onehot(iota((N, m8), 1) // 8 == iota((N, m8), 0)))
    same = iota((m8, m8), 0) % 8 == iota((m8, m8), 1) % 8
    kc_ref[...] = jnp.where(same, full, 0.0).astype(jnp.bfloat16)

    @pl.loop(0, PAIRS)
    def _(pp):
        copy_own(pp).wait()

        @pl.loop(1, DEV)
        def _(k):
            copy_out(pp, (me + k) % DEV).wait_send()

        @pl.loop(1, DEV)
        def _(k):
            src = (me + k) % DEV
            pltpu.make_async_remote_copy(
                src_ref=send.at[pp, src], dst_ref=g_hbm.at[src * PAIRS + pp],
                send_sem=send_sem.at[pp, src], recv_sem=recv_sem.at[pp, src],
                device_id=(frag, src), device_id_type=MESH,
            ).wait_recv()


def last_kernel(main_ref, half_ref, kc_ref, v_ref):
    kc = kc_ref[...]
    k = 8 * N
    for gg in range(2):
        for n in range(2):
            rhs = jnp.concatenate([main_ref[:, gg * 4 + 2 * n + t].reshape(k, 128) for t in range(2)], axis=1)
            out = dot(kc, rhs)
            v_ref[:, gg * 8:(gg + 1) * 8, n * 256:(n + 1) * 256] = out.reshape(N, 8, 256)
    out = dot(kc, half_ref[:, 0].reshape(k, 128))
    v_ref[:, 0:8, 512:576] = out.reshape(N, 8, 128)[:, :, :64]
    v_ref[:, 8:16, 512:576] = pltpu.roll(out, 64, 1).reshape(N, 8, 128)[:, :, :64]


def solution(mesh):
    def local_transform(ao_rows, coeffs):
        blocks = DEV * PAIRS
        g_all, kc = pl.pallas_call(
            exchange_kernel,
            out_shape=(jax.ShapeDtypeStruct((blocks, TILES, 16, 128), jnp.bfloat16),
                       jax.ShapeDtypeStruct((8 * N, 8 * N), jnp.bfloat16)),
            in_specs=[pl.BlockSpec(memory_space=pltpu.HBM), pl.BlockSpec(memory_space=pltpu.HBM)],
            out_specs=(pl.BlockSpec(memory_space=pl.ANY), pl.BlockSpec(memory_space=pltpu.VMEM)),
            scratch_shapes=[
                pltpu.VMEM((2 * PAIRS, N, N, N), jnp.bfloat16),
                pltpu.VMEM((N, N), jnp.bfloat16),
                pltpu.VMEM((2, N * QPAD, 128), jnp.float32),
                pltpu.VMEM((PAIRS, DEV, TILES, 16, 128), jnp.bfloat16),
                pltpu.VMEM((2 * N, 2 * N), jnp.bfloat16),
                pltpu.SemaphoreType.DMA((2 * PAIRS, 4)),
                pltpu.SemaphoreType.DMA,
                pltpu.SemaphoreType.DMA((PAIRS, DEV)),
                pltpu.SemaphoreType.DMA((PAIRS, DEV)),
                pltpu.SemaphoreType.DMA((PAIRS,)),
            ],
            compiler_params=pltpu.CompilerParams(collective_id=0, has_side_effects=True, vmem_limit_bytes=41 * 2**20),
            cost_estimate=pl.CostEstimate(flops=6 * 10**9, bytes_accessed=40 * 10**6, transcendentals=0),
            name='exchange',
        )(ao_rows, coeffs)
        return pl.pallas_call(
            last_kernel,
            grid=(6,),
            out_shape=jax.ShapeDtypeStruct((N, N, COLS * N), jnp.float32),
            in_specs=[
                pl.BlockSpec((blocks, 8, 16, 128), lambda u: (0, u, 0, 0)),
                pl.BlockSpec((blocks, 1, 16, 128), lambda u: (0, 48 + u, 0, 0)),
                pl.BlockSpec((8 * N, 8 * N), lambda u: (0, 0)),
            ],
            out_specs=pl.BlockSpec((N, 16, COLS * N), lambda u: (0, u, 0)),
            compiler_params=pltpu.CompilerParams(vmem_limit_bytes=20 * 2**20),
            cost_estimate=pl.CostEstimate(flops=8 * 10**9, bytes_accessed=35 * 10**6, transcendentals=0),
            name='last_product',
        )(g_all, g_all, kc)

    return jax.shard_map(local_transform, mesh=mesh, in_specs=(P(('frag', 'dev')), P('frag')), out_specs=P('frag', None, 'dev'), check_vma=False)
```

```python
import functools

import jax
import jax.numpy as jnp
from jax import lax
from jax.experimental import pallas as pl
from jax.experimental.pallas import tpu as pltpu
from jax.sharding import PartitionSpec as P

MESH = pl.DeviceIdType.MESH
N = 96
DEV = 16
PAIRS = 3
COLS = 6
QPAD = 104
QB = 8
TILES = 54


def iota(shape, dim):
    return lax.broadcasted_iota(jnp.int32, shape, dim)


def onehot(mask):
    return jnp.where(mask, 1.0, 0.0).astype(jnp.bfloat16)


def dot(x, y, dims=((1,), (0,))):
    return lax.dot_general(x, y, (dims, ((), ())), preferred_element_type=jnp.float32)


def exchange_kernel(a_hbm, c_hbm, g_hbm, kc_ref, a_vm, c_vm, h_scr, send, cc_ref, a_sem, c_sem, send_sem, recv_sem, own_sem):
    frag = lax.axis_index('frag')
    me = lax.axis_index('dev')
    chip, core = me // 2, me % 2
    cz1, cz0, cy = chip // 4, (chip // 2) % 2, chip % 2
    edge = 1 - (cz1 + cz0) % 2

    def load(p, part):
        quarter = pl.ds(part * (N // 4), N // 4)
        return pltpu.make_async_copy(a_hbm.at[p, quarter], a_vm.at[p, quarter], a_sem.at[p, part])

    load_c = pltpu.make_async_copy(c_hbm, c_vm, c_sem)
    load_c.start()
    for p in range(2 * PAIRS):
        for part in range(4):
            load(p, part).start()

    barrier = pltpu.get_barrier_semaphore()

    @pl.loop(1, DEV)
    def _(k):
        pl.semaphore_signal(barrier, inc=1, device_id=(frag, (me + k) % DEV), device_id_type=MESH)

    load_c.wait()
    c = c_vm[...]
    eye = onehot(iota((N, N), 0) == iota((N, N), 1))
    ct = dot(eye, c, ((1,), (1,))).astype(jnp.bfloat16)
    r2, c2 = iota((256, N), 0), iota((N, 256), 1)
    stacked = dot(onehot(r2 % 128 == iota((256, N), 1)), c).astype(jnp.bfloat16)
    both = dot(stacked, onehot(c2 % 128 == iota((N, 256), 0)))
    c_two = jnp.where(iota((256, 256), 0) // 128 == iota((256, 256), 1) // 128, both, 0.0).astype(jnp.bfloat16)
    gap = jnp.zeros((N, 32), jnp.bfloat16)
    row = iota((2 * N, N), 0)
    pick_a = onehot(iota((2 * N, N), 1) == 8 * (row // 16) + row % 8)
    c_rows = dot(pick_a, c, ((1,), (1,))).astype(jnp.bfloat16)
    wide = dot(c_rows, onehot(iota((N, 2 * N), 1) % N == iota((N, 2 * N), 0)))
    same_p = (iota((2 * N, 2 * N), 0) % 16) // 8 == iota((2 * N, 2 * N), 1) // N
    cc_ref[...] = jnp.where(same_p, wide, 0.0).astype(jnp.bfloat16)

    pl.semaphore_wait(barrier, DEV - 1)

    lane = iota((N, 128), 1)

    def copy_out(pp, dest):
        return pltpu.make_async_remote_copy(
            src_ref=send.at[pp, dest],
            dst_ref=g_hbm.at[me * PAIRS + pp],
            send_sem=send_sem.at[pp, dest],
            recv_sem=recv_sem.at[pp, me],
            device_id=(frag, dest),
            device_id_type=MESH,
        )

    def chip_at(m):
        return 4 * ((cz1 + m // 4) % 2) + 2 * ((cz0 + (m // 2) % 2) % 2) + (cy + m % 2) % 2

    def far(n):
        return copy_out(n // 8, chip_at(7 - (n // 2) % 4) * 2 + n % 2)

    def near(n):
        return copy_out(n // 4, chip_at(3 - (n // 2) % 2) * 2 + n % 2)

    def copy_own(pp):
        return pltpu.make_async_copy(send.at[pp, me], g_hbm.at[me * PAIRS + pp], own_sem.at[pp])

    def pack(pp, dest_chip):
        halves = []
        for p in range(2):
            tiles, last = [], []
            for cc in range(2):
                j0 = (dest_chip * 2 + cc) * COLS
                x = [h_scr[p, pl.ds(pl.multiple_of((j0 + l) * QPAD, 8), N), :] for l in range(COLS)]
                r1, r2, r3 = pltpu.roll(x[1], 96, 1), pltpu.roll(x[2], 64, 1), pltpu.roll(x[3], 32, 1)
                r5 = pltpu.roll(x[5], 96, 1)
                tiles += [jnp.where(lane < 96, x[0], r1), jnp.where(lane < 64, r1, r2),
                          jnp.where(lane < 32, r2, r3), jnp.where(lane < 96, x[4], r5)]
                last.append(r5 if cc == 0 else pltpu.roll(x[5], 32, 1))
            tiles.append(jnp.where(lane < 64, last[0], last[1]))
            halves.append(jnp.concatenate([t.astype(jnp.bfloat16) for t in tiles], axis=1))
        rhs = jnp.concatenate(halves, axis=0)
        out = dot(cc_ref[...], rhs)
        for cc in range(2):
            dest = dest_chip * 2 + cc
            for t in range(4):
                tile = out[:, (cc * 4 + t) * 128:(cc * 4 + t + 1) * 128].astype(jnp.bfloat16)
                for g in range(12):
                    send[pp, dest, g * 4 + t] = tile[g * 16:(g + 1) * 16]
        low = iota((16, 128), 1) < 64
        for u in range(6):
            upper = out[u * 32:u * 32 + 16, 1024:]
            lower = out[u * 32 + 16:u * 32 + 32, 1024:]
            send[pp, dest_chip * 2, 48 + u] = jnp.where(low, upper, pltpu.roll(lower, 64, 1)).astype(jnp.bfloat16)
            send[pp, dest_chip * 2 + 1, 48 + u] = jnp.where(low, pltpu.roll(upper, 64, 1), lower).astype(jnp.bfloat16)

    @pl.loop(0, PAIRS)
    def _(pp):
        for p2 in range(2):
            p = pp * 2 + p2
            for part in range(4):
                load(p, part).wait()

                @pl.loop(0, N // 4 // QB)
                def _(qb):
                    q0 = part * (N // 4) + qb * QB
                    t_rows = []
                    for i in range(0, QB, 2):
                        two = jnp.concatenate([a_vm[p, q0 + i], gap, a_vm[p, q0 + i + 1], gap], axis=1)
                        t_rows.append(dot(ct, two).astype(jnp.bfloat16))
                    half = dot(jnp.concatenate(t_rows, axis=0), c_two)
                    for i in range(QB):
                        rows = half[(i // 2) * N:(i // 2 + 1) * N, (i % 2) * 128:(i % 2 + 1) * 128]
                        h_scr[p2, pl.ds(q0 + i, N, stride=QPAD), :] = rows

        @pl.loop(0, 8)
        def _(t):
            m = (7 - t + 4 * edge) % 8
            dest_chip = chip_at(m)
            pack(pp, dest_chip)
            later = (1 - edge) * (m // 2) == 1
            for cc in range(2):
                dest = dest_chip * 2 + cc

                @pl.when(jnp.logical_and(dest != me, jnp.logical_not(later)))
                def _():
                    copy_out(pp, dest).start()

                @pl.when(dest == me)
                def _():
                    copy_own(pp).start()

    m8 = 8 * N
    spread = dot(onehot(iota((m8, N), 0) // 8 == iota((m8, N), 1)), c, ((1,), (1,))).astype(jnp.bfloat16)
    full = dot(spread, onehot(iota((N, m8), 1) // 8 == iota((N, m8), 0)))
    same = iota((m8, m8), 0) % 8 == iota((m8, m8), 1) % 8
    kc_ref[...] = jnp.where(same, full, 0.0).astype(jnp.bfloat16)

    @pl.loop(0, 4 * PAIRS)
    def _(n):
        @pl.when(jnp.logical_and(edge == 0, core == 0))
        def _():
            near(n).start()

        far(2 * n).wait_send()

        @pl.when(jnp.logical_and(edge == 0, core == 1))
        def _():
            near(n).start()

        far(2 * n + 1).wait_send()

    @pl.loop(0, PAIRS)
    def _(pp):
        copy_own(pp).wait()
        copy_out(pp, chip * 2 + 1 - core).wait_send()
        copy_out(pp, chip_at(1) * 2).wait_send()
        copy_out(pp, chip_at(1) * 2 + 1).wait_send()

        @pl.loop(0, 4)
        def _(n):
            near(4 * pp + n).wait_send()

        @pl.loop(1, DEV)
        def _(k):
            src = (me + k) % DEV
            pltpu.make_async_remote_copy(
                src_ref=send.at[pp, src], dst_ref=g_hbm.at[src * PAIRS + pp],
                send_sem=send_sem.at[pp, src], recv_sem=recv_sem.at[pp, src],
                device_id=(frag, src), device_id_type=MESH,
            ).wait_recv()


def last_kernel(main_ref, half_ref, kc_ref, v_ref):
    kc = kc_ref[...]
    k = 8 * N
    for gg in range(2):
        for n in range(2):
            rhs = jnp.concatenate([main_ref[:, gg * 4 + 2 * n + t].reshape(k, 128) for t in range(2)], axis=1)
            out = dot(kc, rhs)
            v_ref[:, gg * 8:(gg + 1) * 8, n * 256:(n + 1) * 256] = out.reshape(N, 8, 256)
    out = dot(kc, half_ref[:, 0].reshape(k, 128))
    v_ref[:, 0:8, 512:576] = out.reshape(N, 8, 128)[:, :, :64]
    v_ref[:, 8:16, 512:576] = pltpu.roll(out, 64, 1).reshape(N, 8, 128)[:, :, :64]


def solution(mesh):
    def local_transform(ao_rows, coeffs):
        blocks = DEV * PAIRS
        g_all, kc = pl.pallas_call(
            exchange_kernel,
            out_shape=(jax.ShapeDtypeStruct((blocks, TILES, 16, 128), jnp.bfloat16),
                       jax.ShapeDtypeStruct((8 * N, 8 * N), jnp.bfloat16)),
            in_specs=[pl.BlockSpec(memory_space=pltpu.HBM), pl.BlockSpec(memory_space=pltpu.HBM)],
            out_specs=(pl.BlockSpec(memory_space=pl.ANY), pl.BlockSpec(memory_space=pltpu.VMEM)),
            scratch_shapes=[
                pltpu.VMEM((2 * PAIRS, N, N, N), jnp.bfloat16),
                pltpu.VMEM((N, N), jnp.bfloat16),
                pltpu.VMEM((2, N * QPAD, 128), jnp.float32),
                pltpu.VMEM((PAIRS, DEV, TILES, 16, 128), jnp.bfloat16),
                pltpu.VMEM((2 * N, 2 * N), jnp.bfloat16),
                pltpu.SemaphoreType.DMA((2 * PAIRS, 4)),
                pltpu.SemaphoreType.DMA,
                pltpu.SemaphoreType.DMA((PAIRS, DEV)),
                pltpu.SemaphoreType.DMA((PAIRS, DEV)),
                pltpu.SemaphoreType.DMA((PAIRS,)),
            ],
            compiler_params=pltpu.CompilerParams(collective_id=0, has_side_effects=True, vmem_limit_bytes=41 * 2**20),
            cost_estimate=pl.CostEstimate(flops=6 * 10**9, bytes_accessed=40 * 10**6, transcendentals=0),
            name='exchange',
        )(ao_rows, coeffs)
        return pl.pallas_call(
            last_kernel,
            grid=(6,),
            out_shape=jax.ShapeDtypeStruct((N, N, COLS * N), jnp.float32),
            in_specs=[
                pl.BlockSpec((blocks, 8, 16, 128), lambda u: (0, u, 0, 0)),
                pl.BlockSpec((blocks, 1, 16, 128), lambda u: (0, 48 + u, 0, 0)),
                pl.BlockSpec((8 * N, 8 * N), lambda u: (0, 0)),
            ],
            out_specs=pl.BlockSpec((N, 16, COLS * N), lambda u: (0, u, 0)),
            compiler_params=pltpu.CompilerParams(vmem_limit_bytes=20 * 2**20),
            cost_estimate=pl.CostEstimate(flops=8 * 10**9, bytes_accessed=35 * 10**6, transcendentals=0),
            name='last_product',
        )(g_all, g_all, kc)

    return jax.shard_map(local_transform, mesh=mesh, in_specs=(P(('frag', 'dev')), P('frag')), out_specs=P('frag', None, 'dev'), check_vma=False)
```

```python
import functools

import jax
import jax.numpy as jnp
from jax import lax
from jax.experimental import pallas as pl
from jax.experimental.pallas import tpu as pltpu
from jax.sharding import PartitionSpec as P

MESH = pl.DeviceIdType.MESH
N = 96
DEV = 16
PAIRS = 3
COLS = 6
QPAD = 104
QB = 8
TILES = 54
PART = 9
GROUPS = ((7, 4, 3, 1), (6, 5, 2, 0))


def iota(shape, dim):
    return lax.broadcasted_iota(jnp.int32, shape, dim)


def onehot(mask):
    return jnp.where(mask, 1.0, 0.0).astype(jnp.bfloat16)


def dot(x, y, dims=((1,), (0,))):
    return lax.dot_general(x, y, (dims, ((), ())), preferred_element_type=jnp.float32)


def exchange_kernel(a_hbm, c_hbm, g_hbm, kc_ref, a_vm, c_vm, h_scr, send, cc_ref, a_sem, c_sem, send_sem, recv_sem, own_sem):
    frag = lax.axis_index('frag')
    me = lax.axis_index('dev')
    chip, core = me // 2, me % 2
    cz1, cz0, cy = chip // 4, (chip // 2) % 2, chip % 2

    def load(p, part):
        quarter = pl.ds(part * (N // 4), N // 4)
        return pltpu.make_async_copy(a_hbm.at[p, quarter], a_vm.at[p, quarter], a_sem.at[p, part])

    load_c = pltpu.make_async_copy(c_hbm, c_vm, c_sem)
    load_c.start()
    for p in range(2 * PAIRS):
        for part in range(4):
            load(p, part).start()

    barrier = pltpu.get_barrier_semaphore()

    @pl.loop(1, DEV)
    def _(k):
        pl.semaphore_signal(barrier, inc=1, device_id=(frag, (me + k) % DEV), device_id_type=MESH)

    load_c.wait()
    c = c_vm[...]
    eye = onehot(iota((N, N), 0) == iota((N, N), 1))
    ct = dot(eye, c, ((1,), (1,))).astype(jnp.bfloat16)
    r2, c2 = iota((256, N), 0), iota((N, 256), 1)
    stacked = dot(onehot(r2 % 128 == iota((256, N), 1)), c).astype(jnp.bfloat16)
    both = dot(stacked, onehot(c2 % 128 == iota((N, 256), 0)))
    c_two = jnp.where(iota((256, 256), 0) // 128 == iota((256, 256), 1) // 128, both, 0.0).astype(jnp.bfloat16)
    gap = jnp.zeros((N, 32), jnp.bfloat16)
    row = iota((2 * N, N), 0)
    pick_a = onehot(iota((2 * N, N), 1) == 8 * (row // 16) + row % 8)
    c_rows = dot(pick_a, c, ((1,), (1,))).astype(jnp.bfloat16)
    wide = dot(c_rows, onehot(iota((N, 2 * N), 1) % N == iota((N, 2 * N), 0)))
    same_p = (iota((2 * N, 2 * N), 0) % 16) // 8 == iota((2 * N, 2 * N), 1) // N
    cc_ref[...] = jnp.where(same_p, wide, 0.0).astype(jnp.bfloat16)

    pl.semaphore_wait(barrier, DEV - 1)

    lane = iota((N, 128), 1)

    def chip_at(m):
        return 4 * ((cz1 + m // 4) % 2) + 2 * ((cz0 + (m // 2) % 2) % 2) + (cy + m % 2) % 2

    def copy_out(pp, dest, part=None):
        tiles = pl.ds(0, TILES) if part is None else pl.ds(part * PART, PART)
        return pltpu.make_async_remote_copy(
            src_ref=send.at[pp, dest, tiles],
            dst_ref=g_hbm.at[me * PAIRS + pp, tiles],
            send_sem=send_sem.at[pp, dest],
            recv_sem=recv_sem.at[pp, me],
            device_id=(frag, dest),
            device_id_type=MESH,
        )

    def copy_own(pp):
        return pltpu.make_async_copy(send.at[pp, me], g_hbm.at[me * PAIRS + pp], own_sem.at[pp])

    def pack(pp, dest_chip):
        halves = []
        for p in range(2):
            tiles, last = [], []
            for cc in range(2):
                j0 = (dest_chip * 2 + cc) * COLS
                x = [h_scr[p, pl.ds(pl.multiple_of((j0 + l) * QPAD, 8), N), :] for l in range(COLS)]
                r1, r2, r3 = pltpu.roll(x[1], 96, 1), pltpu.roll(x[2], 64, 1), pltpu.roll(x[3], 32, 1)
                r5 = pltpu.roll(x[5], 96, 1)
                tiles += [jnp.where(lane < 96, x[0], r1), jnp.where(lane < 64, r1, r2),
                          jnp.where(lane < 32, r2, r3), jnp.where(lane < 96, x[4], r5)]
                last.append(r5 if cc == 0 else pltpu.roll(x[5], 32, 1))
            tiles.append(jnp.where(lane < 64, last[0], last[1]))
            halves.append(jnp.concatenate([t.astype(jnp.bfloat16) for t in tiles], axis=1))
        rhs = jnp.concatenate(halves, axis=0)
        out = dot(cc_ref[...], rhs)
        for cc in range(2):
            dest = dest_chip * 2 + cc
            for t in range(4):
                tile = out[:, (cc * 4 + t) * 128:(cc * 4 + t + 1) * 128].astype(jnp.bfloat16)
                for g in range(12):
                    send[pp, dest, g * 4 + t] = tile[g * 16:(g + 1) * 16]
        low = iota((16, 128), 1) < 64
        for u in range(6):
            upper = out[u * 32:u * 32 + 16, 1024:]
            lower = out[u * 32 + 16:u * 32 + 32, 1024:]
            send[pp, dest_chip * 2, 48 + u] = jnp.where(low, upper, pltpu.roll(lower, 64, 1)).astype(jnp.bfloat16)
            send[pp, dest_chip * 2 + 1, 48 + u] = jnp.where(low, pltpu.roll(upper, 64, 1), lower).astype(jnp.bfloat16)

    @pl.loop(0, PAIRS)
    def _(pp):
        for p2 in range(2):
            p = pp * 2 + p2
            for part in range(4):
                load(p, part).wait()

                @pl.loop(0, N // 4 // QB)
                def _(qb):
                    q0 = part * (N // 4) + qb * QB
                    t_rows = []
                    for i in range(0, QB, 2):
                        two = jnp.concatenate([a_vm[p, q0 + i], gap, a_vm[p, q0 + i + 1], gap], axis=1)
                        t_rows.append(dot(ct, two).astype(jnp.bfloat16))
                    half = dot(jnp.concatenate(t_rows, axis=0), c_two)
                    for i in range(QB):
                        rows = half[(i // 2) * N:(i // 2 + 1) * N, (i % 2) * 128:(i % 2 + 1) * 128]
                        h_scr[p2, pl.ds(q0 + i, N, stride=QPAD), :] = rows

        for group in GROUPS:
            for m in group:
                pack(pp, chip_at(m))

            @pl.loop(0, TILES // PART)
            def _(part):
                for cc in range(2):
                    for m in group:
                        if m > 0:
                            copy_out(pp, chip_at(m) * 2 + cc, part).start()
                        elif cc == 1:
                            copy_out(pp, chip * 2 + 1 - core, part).start()

        copy_own(pp).start()

    m8 = 8 * N
    spread = dot(onehot(iota((m8, N), 0) // 8 == iota((m8, N), 1)), c, ((1,), (1,))).astype(jnp.bfloat16)
    full = dot(spread, onehot(iota((N, m8), 1) // 8 == iota((N, m8), 0)))
    same = iota((m8, m8), 0) % 8 == iota((m8, m8), 1) % 8
    kc_ref[...] = jnp.where(same, full, 0.0).astype(jnp.bfloat16)

    @pl.loop(0, PAIRS)
    def _(pp):
        copy_own(pp).wait()

        @pl.loop(1, DEV)
        def _(k):
            copy_out(pp, (me + k) % DEV).wait_send()

        @pl.loop(1, DEV)
        def _(k):
            src = (me + k) % DEV
            pltpu.make_async_remote_copy(
                src_ref=send.at[pp, src], dst_ref=g_hbm.at[src * PAIRS + pp],
                send_sem=send_sem.at[pp, src], recv_sem=recv_sem.at[pp, src],
                device_id=(frag, src), device_id_type=MESH,
            ).wait_recv()


def last_kernel(main_ref, half_ref, kc_ref, v_ref):
    kc = kc_ref[...]
    k = 8 * N
    for gg in range(2):
        for n in range(2):
            rhs = jnp.concatenate([main_ref[:, gg * 4 + 2 * n + t].reshape(k, 128) for t in range(2)], axis=1)
            out = dot(kc, rhs)
            v_ref[:, gg * 8:(gg + 1) * 8, n * 256:(n + 1) * 256] = out.reshape(N, 8, 256)
    out = dot(kc, half_ref[:, 0].reshape(k, 128))
    v_ref[:, 0:8, 512:576] = out.reshape(N, 8, 128)[:, :, :64]
    v_ref[:, 8:16, 512:576] = pltpu.roll(out, 64, 1).reshape(N, 8, 128)[:, :, :64]


def solution(mesh):
    def local_transform(ao_rows, coeffs):
        blocks = DEV * PAIRS
        g_all, kc = pl.pallas_call(
            exchange_kernel,
            out_shape=(jax.ShapeDtypeStruct((blocks, TILES, 16, 128), jnp.bfloat16),
                       jax.ShapeDtypeStruct((8 * N, 8 * N), jnp.bfloat16)),
            in_specs=[pl.BlockSpec(memory_space=pltpu.HBM), pl.BlockSpec(memory_space=pltpu.HBM)],
            out_specs=(pl.BlockSpec(memory_space=pl.ANY), pl.BlockSpec(memory_space=pltpu.VMEM)),
            scratch_shapes=[
                pltpu.VMEM((2 * PAIRS, N, N, N), jnp.bfloat16),
                pltpu.VMEM((N, N), jnp.bfloat16),
                pltpu.VMEM((2, N * QPAD, 128), jnp.float32),
                pltpu.VMEM((PAIRS, DEV, TILES, 16, 128), jnp.bfloat16),
                pltpu.VMEM((2 * N, 2 * N), jnp.bfloat16),
                pltpu.SemaphoreType.DMA((2 * PAIRS, 4)),
                pltpu.SemaphoreType.DMA,
                pltpu.SemaphoreType.DMA((PAIRS, DEV)),
                pltpu.SemaphoreType.DMA((PAIRS, DEV)),
                pltpu.SemaphoreType.DMA((PAIRS,)),
            ],
            compiler_params=pltpu.CompilerParams(collective_id=0, has_side_effects=True, vmem_limit_bytes=41 * 2**20),
            cost_estimate=pl.CostEstimate(flops=6 * 10**9, bytes_accessed=40 * 10**6, transcendentals=0),
            name='exchange',
        )(ao_rows, coeffs)
        return pl.pallas_call(
            last_kernel,
            grid=(6,),
            out_shape=jax.ShapeDtypeStruct((N, N, COLS * N), jnp.float32),
            in_specs=[
                pl.BlockSpec((blocks, 8, 16, 128), lambda u: (0, u, 0, 0)),
                pl.BlockSpec((blocks, 1, 16, 128), lambda u: (0, 48 + u, 0, 0)),
                pl.BlockSpec((8 * N, 8 * N), lambda u: (0, 0)),
            ],
            out_specs=pl.BlockSpec((N, 16, COLS * N), lambda u: (0, u, 0)),
            compiler_params=pltpu.CompilerParams(vmem_limit_bytes=20 * 2**20),
            cost_estimate=pl.CostEstimate(flops=8 * 10**9, bytes_accessed=35 * 10**6, transcendentals=0),
            name='last_product',
        )(g_all, g_all, kc)

    return jax.shard_map(local_transform, mesh=mesh, in_specs=(P(('frag', 'dev')), P('frag')), out_specs=P('frag', None, 'dev'), check_vma=False)
```

```python
import jax
import jax.numpy as jnp
from jax import lax
from jax.experimental import pallas as pl
from jax.experimental.pallas import tpu as pltpu
from jax.sharding import PartitionSpec as P

MESH = pl.DeviceIdType.MESH
N = 96
DEV = 16
PAIRS = 3
COLS = 6
QPAD = 104
QB = 24
TILES = 54
PART = 9
K8 = 8 * N
KP = 16 * DEV
FIRST_GROUPS = ((7, 4), (6, 5), (3, 1), (2, 0))
LATER_GROUPS = ((7, 4, 3, 1, 6, 5, 2, 0),)


def iota(shape, dim):
    return lax.broadcasted_iota(jnp.int32, shape, dim)


def onehot(mask):
    return jnp.where(mask, 1.0, 0.0).astype(jnp.bfloat16)


def dot(x, y, dims=((1,), (0,))):
    return lax.dot_general(x, y, (dims, ((), ())), preferred_element_type=jnp.float32)


def exchange_kernel(a_hbm, c_hbm, g_last, vm0_ref, vm1_ref, vm2_ref, vh_ref, kc_ref,
                    a_vm, c_vm, h_scr, send, g_first, cc_ref, kc_first, a_sem, c_sem, send_sem, recv_sem, own_sem):
    frag = lax.axis_index('frag')
    me = lax.axis_index('dev')
    chip, core = me // 2, me % 2
    cz1, cz0, cy = chip // 4, (chip // 2) % 2, chip % 2

    def load(pp, idx):
        p2, quarter = idx // 4, pl.ds((idx % 4) * QB, QB)
        return pltpu.make_async_copy(a_hbm.at[2 * pp + p2, quarter], a_vm.at[p2, quarter], a_sem.at[idx])

    load_c = pltpu.make_async_copy(c_hbm, c_vm, c_sem)
    load_c.start()
    for idx in range(8):
        load(0, idx).start()

    barrier = pltpu.get_barrier_semaphore()

    @pl.loop(1, DEV)
    def _(k):
        pl.semaphore_signal(barrier, inc=1, device_id=(frag, (me + k) % DEV), device_id_type=MESH)

    load_c.wait()
    c = c_vm[...]
    eye = onehot(iota((N, N), 0) == iota((N, N), 1))
    ct = dot(eye, c, ((1,), (1,))).astype(jnp.bfloat16)
    stacked = dot(onehot(iota((256, N), 0) % 128 == iota((256, N), 1)), c).astype(jnp.bfloat16)
    both = dot(stacked, onehot(iota((N, 256), 1) % 128 == iota((N, 256), 0)))
    c_two = jnp.where(iota((256, 256), 0) // 128 == iota((256, 256), 1) // 128, both, 0.0).astype(jnp.bfloat16)
    gap = jnp.zeros((N, 32), jnp.bfloat16)
    row = iota((2 * N, N), 0)
    pick_a = onehot(iota((2 * N, N), 1) == 8 * (row // 16) + row % 8)
    c_rows = dot(pick_a, c, ((1,), (1,))).astype(jnp.bfloat16)
    wide = dot(c_rows, onehot(iota((N, 2 * N), 1) % N == iota((N, 2 * N), 0)))
    same_p = (iota((2 * N, 2 * N), 0) % 16) // 8 == iota((2 * N, 2 * N), 1) // N
    cc_ref[...] = jnp.where(same_p, wide, 0.0).astype(jnp.bfloat16)

    lane = iota((N, 128), 1)

    def chip_at(m):
        return 4 * ((cz1 + m // 4) % 2) + 2 * ((cz0 + (m // 2) % 2) % 2) + (cy + m % 2) % 2

    def block(pp, src, tiles):
        if isinstance(pp, int) and pp == PAIRS - 1:
            return g_last.at[src, tiles]
        return g_first.at[pp, src, tiles]

    def copy_out(pp, dest, part=None):
        tiles = pl.ds(0, TILES) if part is None else pl.ds(part * PART, PART)
        return pltpu.make_async_remote_copy(
            src_ref=send.at[pp, dest, tiles],
            dst_ref=block(pp, me, tiles),
            send_sem=send_sem.at[pp, dest],
            recv_sem=recv_sem.at[pp, me],
            device_id=(frag, dest),
            device_id_type=MESH,
        )

    def wait_recv(pp, src):
        tiles = pl.ds(0, TILES)
        pltpu.make_async_remote_copy(
            src_ref=send.at[pp, src, tiles], dst_ref=block(pp, src, tiles),
            send_sem=send_sem.at[pp, src], recv_sem=recv_sem.at[pp, src],
            device_id=(frag, src), device_id_type=MESH,
        ).wait_recv()

    def half_transform(pp):
        @pl.loop(0, 8)
        def _(idx):
            load(pp, idx).wait()
            p2, q0 = idx // 4, (idx % 4) * QB
            t_rows = []
            for i in range(0, QB, 2):
                two = jnp.concatenate([a_vm[p2, q0 + i], gap, a_vm[p2, q0 + i + 1], gap], axis=1)
                t_rows.append(dot(ct, two).astype(jnp.bfloat16))
            half = dot(jnp.concatenate(t_rows, axis=0), c_two)
            for i in range(QB):
                rows = half[(i // 2) * N:(i // 2 + 1) * N, (i % 2) * 128:(i % 2 + 1) * 128]
                h_scr[p2, pl.ds(q0 + i, N, stride=QPAD), :] = rows

    def pack(pp, dest_chip):
        halves = []
        for p in range(2):
            tiles, last = [], []
            for cc in range(2):
                j0 = (dest_chip * 2 + cc) * COLS
                x = [h_scr[p, pl.ds(pl.multiple_of((j0 + l) * QPAD, 8), N), :] for l in range(COLS)]
                r1, r2, r3 = pltpu.roll(x[1], 96, 1), pltpu.roll(x[2], 64, 1), pltpu.roll(x[3], 32, 1)
                r5 = pltpu.roll(x[5], 96, 1)
                tiles += [jnp.where(lane < 96, x[0], r1), jnp.where(lane < 64, r1, r2),
                          jnp.where(lane < 32, r2, r3), jnp.where(lane < 96, x[4], r5)]
                last.append(r5 if cc == 0 else pltpu.roll(x[5], 32, 1))
            tiles.append(jnp.where(lane < 64, last[0], last[1]))
            halves.append(jnp.concatenate([t.astype(jnp.bfloat16) for t in tiles], axis=1))
        out = dot(cc_ref[...], jnp.concatenate(halves, axis=0))
        for cc in range(2):
            dest = dest_chip * 2 + cc
            for t in range(4):
                tile = out[:, (cc * 4 + t) * 128:(cc * 4 + t + 1) * 128].astype(jnp.bfloat16)
                for g in range(12):
                    send[pp, dest, g * 4 + t] = tile[g * 16:(g + 1) * 16]
        low = iota((16, 128), 1) < 64
        for u in range(6):
            upper = out[u * 32:u * 32 + 16, 1024:]
            lower = out[u * 32 + 16:u * 32 + 32, 1024:]
            send[pp, dest_chip * 2, 48 + u] = jnp.where(low, upper, pltpu.roll(lower, 64, 1)).astype(jnp.bfloat16)
            send[pp, dest_chip * 2 + 1, 48 + u] = jnp.where(low, pltpu.roll(upper, 64, 1), lower).astype(jnp.bfloat16)

    def send_groups(pp, groups):
        for group in groups:
            for m in group:
                pack(pp, chip_at(m))

            @pl.loop(0, TILES // PART)
            def _(part):
                for cc in range(2):
                    for m in group:
                        if m > 0:
                            copy_out(pp, chip_at(m) * 2 + cc, part).start()
                        elif cc == 1:
                            copy_out(pp, chip * 2 + 1 - core, part).start()

    def copy_own(pp):
        return pltpu.make_async_copy(send.at[pp, me], block(pp, me, pl.ds(0, TILES)), own_sem.at[pp])

    half_transform(0)
    for idx in range(8):
        load(1, idx).start()
    pl.semaphore_wait(barrier, DEV - 1)
    send_groups(0, FIRST_GROUPS)
    copy_own(0).start()
    for pp in range(1, PAIRS):
        half_transform(pp)
        if pp < PAIRS - 1:
            for idx in range(8):
                load(pp + 1, idx).start()
        send_groups(pp, LATER_GROUPS)
        copy_own(pp).start()

    spread = dot(onehot(iota((K8, N), 0) // 8 == iota((K8, N), 1)), c, ((1,), (1,))).astype(jnp.bfloat16)
    col, p_row = iota((N, KP), 1), iota((N, KP), 0)
    same = iota((K8, KP), 0) % 8 == iota((K8, KP), 1) % 8
    for pp in range(PAIRS):
        full = dot(spread, onehot(p_row == (col // 16) * COLS + 2 * pp + (col % 16) // 8))
        kc = jnp.where(same, full, 0.0).astype(jnp.bfloat16)
        if pp < PAIRS - 1:
            kc_first[:, pp * KP:(pp + 1) * KP] = kc
        else:
            kc_ref[...] = kc

    for pp in range(PAIRS - 1):
        copy_own(pp).wait()

        @pl.loop(1, DEV)
        def _(k):
            wait_recv(pp, (me + k) % DEV)

    def rhs_first(tile):
        return jnp.concatenate([g_first[pp, :, tile].reshape(KP, 128) for pp in range(PAIRS - 1)], axis=0)

    for third, vm_ref in enumerate((vm0_ref, vm1_ref, vm2_ref)):
        @pl.loop(0, 4)
        def _(g):
            for n in range(2):
                rhs = jnp.concatenate([rhs_first((4 * third + g) * 4 + 2 * n + t) for t in range(2)], axis=1)
                vm_ref[g, :, n * 256:(n + 1) * 256] = dot(kc_first[...], rhs)

    @pl.loop(0, 6)
    def _(u):
        vh_ref[u] = dot(kc_first[...], rhs_first(48 + u))

    for pp in range(PAIRS):
        @pl.loop(1, DEV)
        def _(k):
            copy_out(pp, (me + k) % DEV).wait_send()

    copy_own(PAIRS - 1).wait()

    @pl.loop(1, DEV)
    def _(k):
        wait_recv(PAIRS - 1, (me + k) % DEV)


def last_kernel(g_ref, vm0_ref, vm1_ref, vm2_ref, vh_ref, kc_ref, v_ref):
    u = pl.program_id(0)
    kc = kc_ref[...]
    for third, vm_ref in enumerate((vm0_ref, vm1_ref, vm2_ref)):
        @pl.when(u // 2 == third)
        def _():
            for gg in range(2):
                g = 2 * u + gg
                for n in range(2):
                    rhs = jnp.concatenate([g_ref[:, g * 4 + 2 * n + t].reshape(KP, 128) for t in range(2)], axis=1)
                    out = vm_ref[g - 4 * third, :, n * 256:(n + 1) * 256] + dot(kc, rhs)
                    v_ref[:, gg * 8:(gg + 1) * 8, n * 256:(n + 1) * 256] = out.reshape(N, 8, 256)

    out = vh_ref[u] + dot(kc, g_ref[:, 48 + u].reshape(KP, 128))
    v_ref[:, 0:8, 512:576] = out.reshape(N, 8, 128)[:, :, :64]
    v_ref[:, 8:16, 512:576] = pltpu.roll(out, 64, 1).reshape(N, 8, 128)[:, :, :64]


def solution(mesh):
    def local_transform(ao_rows, coeffs):
        vmem = pl.BlockSpec(memory_space=pltpu.VMEM)
        hbm = pl.BlockSpec(memory_space=pltpu.HBM)
        parts = pl.pallas_call(
            exchange_kernel,
            out_shape=(pltpu.VMEM((DEV, TILES, 16, 128), jnp.bfloat16),
                       *[pltpu.VMEM((4, K8, 512), jnp.float32)] * 3,
                       pltpu.VMEM((6, K8, 128), jnp.float32),
                       pltpu.VMEM((K8, KP), jnp.bfloat16)),
            in_specs=[hbm, hbm],
            out_specs=(vmem,) * 6,
            scratch_shapes=[
                pltpu.VMEM((2, N, N, N), jnp.bfloat16),
                pltpu.VMEM((N, N), jnp.bfloat16),
                pltpu.VMEM((2, N * QPAD, 128), jnp.float32),
                pltpu.VMEM((PAIRS, DEV, TILES, 16, 128), jnp.bfloat16),
                pltpu.VMEM((PAIRS - 1, DEV, TILES, 16, 128), jnp.bfloat16),
                pltpu.VMEM((2 * N, 2 * N), jnp.bfloat16),
                pltpu.VMEM((K8, (PAIRS - 1) * KP), jnp.bfloat16),
                pltpu.SemaphoreType.DMA((8,)),
                pltpu.SemaphoreType.DMA,
                pltpu.SemaphoreType.DMA((PAIRS, DEV)),
                pltpu.SemaphoreType.DMA((PAIRS, DEV)),
                pltpu.SemaphoreType.DMA((PAIRS,)),
            ],
            compiler_params=pltpu.CompilerParams(collective_id=0, has_side_effects=True, vmem_limit_bytes=34 * 2**20),
            cost_estimate=pl.CostEstimate(flops=10**10, bytes_accessed=40 * 10**6, transcendentals=0),
            name='exchange',
        )(*[pltpu.with_memory_space_constraint(x, pltpu.HBM) for x in (ao_rows, coeffs)])
        return pl.pallas_call(
            last_kernel,
            grid=(6,),
            out_shape=jax.ShapeDtypeStruct((N, N, COLS * N), jnp.float32),
            in_specs=[vmem] * 6,
            out_specs=pl.BlockSpec((N, 16, COLS * N), lambda u: (0, u, 0)),
            compiler_params=pltpu.CompilerParams(vmem_limit_bytes=12 * 2**20),
            cost_estimate=pl.CostEstimate(flops=3 * 10**9, bytes_accessed=24 * 10**6, transcendentals=0),
            name='last_product',
        )(*[pltpu.with_memory_space_constraint(x, pltpu.VMEM) for x in parts])

    return jax.shard_map(local_transform, mesh=mesh, in_specs=(P(('frag', 'dev')), P('frag')), out_specs=P('frag', None, 'dev'), check_vma=False)
```

```python
import jax
import jax.numpy as jnp
from jax import lax
from jax.experimental import pallas as pl
from jax.experimental.pallas import tpu as pltpu
from jax.sharding import PartitionSpec as P

MESH = pl.DeviceIdType.MESH
N = 96
DEV = 16
PAIRS = 3
COLS = 6
QPAD = 104
QB = 24
TILES = 54
PART = 9
K8 = 8 * N
KP = 16 * DEV
HEAD = 32
FIRST_GROUPS = ((2, 3), (4, 5, 6, 7))
LATER_GROUPS = ((0, 3, 4, 6, 1, 2, 5, 7),)


def iota(shape, dim):
    return lax.broadcasted_iota(jnp.int32, shape, dim)


def onehot(mask):
    return jnp.where(mask, 1.0, 0.0).astype(jnp.bfloat16)


def dot(x, y, dims=((1,), (0,))):
    return lax.dot_general(x, y, (dims, ((), ())), preferred_element_type=jnp.float32)


def exchange_kernel(a_hbm, c_hbm, g_last, vm0_ref, vm1_ref, vm2_ref, vh_ref, kc_ref,
                    a_vm, c_vm, ct_ref, h_scr, send, g_first, cc_ref, kc_first, a_sem, c_sem, send_sem, recv_sem, own_sem):
    frag = lax.axis_index('frag')
    me = lax.axis_index('dev')
    chip, core = me // 2, me % 2
    cz1, cz0, cy = chip // 4, (chip // 2) % 2, chip % 2

    def chip_of(slot):
        m = 7 - slot
        return 4 * ((cz1 + m // 4) % 2) + 2 * ((cz0 + (m // 2) % 2) % 2) + (cy + m % 2) % 2

    def load(pp, idx):
        p2, quarter = idx // 4, pl.ds((idx % 4) * QB, QB)
        return pltpu.make_async_copy(a_hbm.at[2 * pp + p2, quarter], a_vm.at[p2, quarter], a_sem.at[idx])

    load_c = pltpu.make_async_copy(c_hbm, c_vm, c_sem)
    load_c.start()
    for idx in range(8):
        load(0, idx).start()

    barrier = pltpu.get_barrier_semaphore()

    @pl.loop(1, DEV)
    def _(k):
        pl.semaphore_signal(barrier, inc=1, device_id=(frag, (me + k) % DEV), device_id_type=MESH)

    load_c.wait()
    c = c_vm[...]
    j_row = iota((N, N), 0)
    pick_j = onehot(iota((N, N), 1) == 2 * COLS * chip_of(j_row // (2 * COLS)) + j_row % (2 * COLS))
    ct_ref[...] = dot(pick_j, c, ((1,), (1,))).astype(jnp.bfloat16)
    stacked = dot(onehot(iota((256, N), 0) % 128 == iota((256, N), 1)), c).astype(jnp.bfloat16)
    both = dot(stacked, onehot(iota((N, 256), 1) % 128 == iota((N, 256), 0)))
    c_two = jnp.where(iota((256, 256), 0) // 128 == iota((256, 256), 1) // 128, both, 0.0).astype(jnp.bfloat16)
    gap = jnp.zeros((N, 32), jnp.bfloat16)
    row = iota((2 * N, N), 0)
    pick_a = onehot(iota((2 * N, N), 1) == 8 * (row // 16) + row % 8)
    c_rows = dot(pick_a, c, ((1,), (1,))).astype(jnp.bfloat16)
    wide = dot(c_rows, onehot(iota((N, 2 * N), 1) % N == iota((N, 2 * N), 0)))
    same_p = (iota((2 * N, 2 * N), 0) % 16) // 8 == iota((2 * N, 2 * N), 1) // N
    cc_ref[...] = jnp.where(same_p, wide, 0.0).astype(jnp.bfloat16)

    lane = iota((N, 128), 1)

    def block(pp, src, tiles):
        if isinstance(pp, int) and pp == PAIRS - 1:
            return g_last.at[src, tiles]
        return g_first.at[pp, src, tiles]

    def copy_out(pp, dest, part=None):
        tiles = pl.ds(0, TILES) if part is None else pl.ds(part * PART, PART)
        return pltpu.make_async_remote_copy(
            src_ref=send.at[pp, dest, tiles],
            dst_ref=block(pp, me, tiles),
            send_sem=send_sem.at[pp, dest],
            recv_sem=recv_sem.at[pp, me],
            device_id=(frag, dest),
            device_id_type=MESH,
        )

    def wait_recv(pp, src):
        tiles = pl.ds(0, TILES)
        pltpu.make_async_remote_copy(
            src_ref=send.at[pp, src, tiles], dst_ref=block(pp, src, tiles),
            send_sem=send_sem.at[pp, src], recv_sem=recv_sem.at[pp, src],
            device_id=(frag, src), device_id_type=MESH,
        ).wait_recv()

    def half_transform(pp, first, rows, loads, wait=True):
        @pl.loop(0, 8 // loads)
        def _(step):
            if wait:
                for i in range(loads):
                    load(pp, step * loads + i).wait()
            p2, q0 = step * loads // 4, (step * loads % 4) * QB
            t_rows = []
            for i in range(0, loads * QB, 2):
                two = jnp.concatenate([a_vm[p2, q0 + i], gap, a_vm[p2, q0 + i + 1], gap], axis=1)
                t_rows.append(dot(ct_ref[first:first + rows], two).astype(jnp.bfloat16))
            half = dot(jnp.concatenate(t_rows, axis=0), c_two)
            for i in range(loads * QB):
                part = half[(i // 2) * rows:(i // 2 + 1) * rows, (i % 2) * 128:(i % 2 + 1) * 128]
                h_scr[p2, pl.ds(first * QPAD + q0 + i, rows, stride=QPAD), :] = part

    def pack(pp, slot):
        dest_chip = chip_of(slot)
        halves = []
        for p in range(2):
            tiles, last = [], []
            for cc in range(2):
                j0 = (slot * 2 + cc) * COLS
                x = [h_scr[p, pl.ds((j0 + l) * QPAD, N), :] for l in range(COLS)]
                r1, r2, r3 = pltpu.roll(x[1], 96, 1), pltpu.roll(x[2], 64, 1), pltpu.roll(x[3], 32, 1)
                r5 = pltpu.roll(x[5], 96, 1)
                tiles += [jnp.where(lane < 96, x[0], r1), jnp.where(lane < 64, r1, r2),
                          jnp.where(lane < 32, r2, r3), jnp.where(lane < 96, x[4], r5)]
                last.append(r5 if cc == 0 else pltpu.roll(x[5], 32, 1))
            tiles.append(jnp.where(lane < 64, last[0], last[1]))
            halves.append(jnp.concatenate([t.astype(jnp.bfloat16) for t in tiles], axis=1))
        out = dot(cc_ref[...], jnp.concatenate(halves, axis=0))
        for cc in range(2):
            dest = dest_chip * 2 + cc
            for t in range(4):
                tile = out[:, (cc * 4 + t) * 128:(cc * 4 + t + 1) * 128].astype(jnp.bfloat16)
                for g in range(12):
                    send[pp, dest, g * 4 + t] = tile[g * 16:(g + 1) * 16]
        low = iota((16, 128), 1) < 64
        for u in range(6):
            upper = out[u * 32:u * 32 + 16, 1024:]
            lower = out[u * 32 + 16:u * 32 + 32, 1024:]
            send[pp, dest_chip * 2, 48 + u] = jnp.where(low, upper, pltpu.roll(lower, 64, 1)).astype(jnp.bfloat16)
            send[pp, dest_chip * 2 + 1, 48 + u] = jnp.where(low, pltpu.roll(upper, 64, 1), lower).astype(jnp.bfloat16)

    def send_groups(pp, groups):
        for group in groups:
            for slot in group:
                pack(pp, slot)

            @pl.loop(0, TILES // PART)
            def _(part):
                for cc in range(2):
                    for slot in group:
                        if slot < 7:
                            copy_out(pp, chip_of(slot) * 2 + cc, part).start()
                        elif cc == 1:
                            copy_out(pp, chip * 2 + 1 - core, part).start()

    def copy_own(pp):
        return pltpu.make_async_copy(send.at[pp, me], block(pp, me, pl.ds(0, TILES)), own_sem.at[pp])

    half_transform(0, 0, HEAD, 2)
    pl.semaphore_wait(barrier, DEV - 1)
    send_groups(0, ((0, 1),))
    half_transform(0, HEAD, N - HEAD, 1, wait=False)
    for idx in range(8):
        load(1, idx).start()
    send_groups(0, FIRST_GROUPS)
    copy_own(0).start()
    for pp in range(1, PAIRS):
        half_transform(pp, 0, N, 1)
        if pp < PAIRS - 1:
            for idx in range(8):
                load(pp + 1, idx).start()
        send_groups(pp, LATER_GROUPS)
        copy_own(pp).start()

    spread = dot(onehot(iota((K8, N), 0) // 8 == iota((K8, N), 1)), c, ((1,), (1,))).astype(jnp.bfloat16)
    col, p_row = iota((N, KP), 1), iota((N, KP), 0)
    same = iota((K8, KP), 0) % 8 == iota((K8, KP), 1) % 8
    for pp in range(PAIRS):
        full = dot(spread, onehot(p_row == (col // 16) * COLS + 2 * pp + (col % 16) // 8))
        kc = jnp.where(same, full, 0.0).astype(jnp.bfloat16)
        if pp < PAIRS - 1:
            kc_first[:, pp * KP:(pp + 1) * KP] = kc
        else:
            kc_ref[...] = kc

    for pp in range(PAIRS - 1):
        copy_own(pp).wait()

        @pl.loop(1, DEV)
        def _(k):
            wait_recv(pp, (me + k) % DEV)

    def rhs_first(tile):
        return jnp.concatenate([g_first[pp, :, tile].reshape(KP, 128) for pp in range(PAIRS - 1)], axis=0)

    for third, vm_ref in enumerate((vm0_ref, vm1_ref, vm2_ref)):
        @pl.loop(0, 4)
        def _(g):
            for n in range(2):
                rhs = jnp.concatenate([rhs_first((4 * third + g) * 4 + 2 * n + t) for t in range(2)], axis=1)
                vm_ref[g, :, n * 256:(n + 1) * 256] = dot(kc_first[...], rhs)

    @pl.loop(0, 6)
    def _(u):
        vh_ref[u] = dot(kc_first[...], rhs_first(48 + u))

    for pp in range(PAIRS):
        @pl.loop(1, DEV)
        def _(k):
            copy_out(pp, (me + k) % DEV).wait_send()

    copy_own(PAIRS - 1).wait()

    @pl.loop(1, DEV)
    def _(k):
        wait_recv(PAIRS - 1, (me + k) % DEV)


def last_kernel(g_ref, vm0_ref, vm1_ref, vm2_ref, vh_ref, kc_ref, v_ref):
    g = pl.program_id(0)
    kc = kc_ref[...]
    for third, vm_ref in enumerate((vm0_ref, vm1_ref, vm2_ref)):
        @pl.when(g // 4 == third)
        def _():
            for n in range(2):
                rhs = jnp.concatenate([g_ref[:, g * 4 + 2 * n + t].reshape(KP, 128) for t in range(2)], axis=1)
                out = vm_ref[g - 4 * third, :, n * 256:(n + 1) * 256] + dot(kc, rhs)
                v_ref[:, :, n * 256:(n + 1) * 256] = out.reshape(N, 8, 256)

    both = vh_ref[g // 2] + dot(kc, g_ref[:, 48 + g // 2].reshape(KP, 128))

    @pl.when(g % 2 == 0)
    def _():
        v_ref[:, :, 512:576] = both.reshape(N, 8, 128)[:, :, :64]

    @pl.when(g % 2 == 1)
    def _():
        v_ref[:, :, 512:576] = pltpu.roll(both, 64, 1).reshape(N, 8, 128)[:, :, :64]


def solution(mesh):
    def local_transform(ao_rows, coeffs):
        vmem = pl.BlockSpec(memory_space=pltpu.VMEM)
        hbm = pl.BlockSpec(memory_space=pltpu.HBM)
        parts = pl.pallas_call(
            exchange_kernel,
            out_shape=(pltpu.VMEM((DEV, TILES, 16, 128), jnp.bfloat16),
                       *[pltpu.VMEM((4, K8, 512), jnp.float32)] * 3,
                       pltpu.VMEM((6, K8, 128), jnp.float32),
                       pltpu.VMEM((K8, KP), jnp.bfloat16)),
            in_specs=[hbm, hbm],
            out_specs=(vmem,) * 6,
            scratch_shapes=[
                pltpu.VMEM((2, N, N, N), jnp.bfloat16),
                pltpu.VMEM((N, N), jnp.bfloat16),
                pltpu.VMEM((N, N), jnp.bfloat16),
                pltpu.VMEM((2, N * QPAD, 128), jnp.float32),
                pltpu.VMEM((PAIRS, DEV, TILES, 16, 128), jnp.bfloat16),
                pltpu.VMEM((PAIRS - 1, DEV, TILES, 16, 128), jnp.bfloat16),
                pltpu.VMEM((2 * N, 2 * N), jnp.bfloat16),
                pltpu.VMEM((K8, (PAIRS - 1) * KP), jnp.bfloat16),
                pltpu.SemaphoreType.DMA((8,)),
                pltpu.SemaphoreType.DMA,
                pltpu.SemaphoreType.DMA((PAIRS, DEV)),
                pltpu.SemaphoreType.DMA((PAIRS, DEV)),
                pltpu.SemaphoreType.DMA((PAIRS,)),
            ],
            compiler_params=pltpu.CompilerParams(collective_id=0, has_side_effects=True, vmem_limit_bytes=34 * 2**20),
            cost_estimate=pl.CostEstimate(flops=10**10, bytes_accessed=40 * 10**6, transcendentals=0),
            name='exchange',
        )(*[pltpu.with_memory_space_constraint(x, pltpu.HBM) for x in (ao_rows, coeffs)])
        return pl.pallas_call(
            last_kernel,
            grid=(12,),
            out_shape=jax.ShapeDtypeStruct((N, N, COLS * N), jnp.float32),
            in_specs=[vmem] * 6,
            out_specs=pl.BlockSpec((N, 8, COLS * N), lambda g: (0, g, 0)),
            compiler_params=pltpu.CompilerParams(vmem_limit_bytes=12 * 2**20),
            cost_estimate=pl.CostEstimate(flops=3 * 10**9, bytes_accessed=24 * 10**6, transcendentals=0),
            name='last_product',
        )(*[pltpu.with_memory_space_constraint(x, pltpu.VMEM) for x in parts])

    return jax.shard_map(local_transform, mesh=mesh, in_specs=(P(('frag', 'dev')), P('frag')), out_specs=P('frag', None, 'dev'), check_vma=False)
```

```python
import jax
import jax.numpy as jnp
from jax import lax
from jax.experimental import pallas as pl
from jax.experimental.pallas import tpu as pltpu
from jax.sharding import PartitionSpec as P

MESH = pl.DeviceIdType.MESH
N = 96
DEV = 16
PAIRS = 3
COLS = 6
QPAD = 104
QB = 24
TILES = 54
PART = 9
K8 = 8 * N
KP = 16 * DEV
HEAD = 32
FIRST_GROUPS = ((2, 3), (4, 5, 6, 7))
LATER_GROUPS = ((0, 3, 4, 6, 1, 2, 5, 7),)


def iota(shape, dim):
    return lax.broadcasted_iota(jnp.int32, shape, dim)


def onehot(mask):
    return jnp.where(mask, 1.0, 0.0).astype(jnp.bfloat16)


def dot(x, y, dims=((1,), (0,))):
    return lax.dot_general(x, y, (dims, ((), ())), preferred_element_type=jnp.float32)


def exchange_kernel(a_hbm, c_hbm, g_last, vm0_ref, vm1_ref, vm2_ref, vh_ref, kc_ref,
                    a_vm, c_vm, ct_ref, h_scr, send, g_first, cc_ref, kc_first, a_sem, c_sem, send_sem, recv_sem, own_sem):
    frag = lax.axis_index('frag')
    me = lax.axis_index('dev')
    chip, core = me // 2, me % 2
    cz1, cz0, cy = chip // 4, (chip // 2) % 2, chip % 2

    def chip_of(slot):
        m = 7 - slot
        return 4 * ((cz1 + m // 4) % 2) + 2 * ((cz0 + (m // 2) % 2) % 2) + (cy + m % 2) % 2

    def load(pp, idx):
        p2, quarter = idx // 4, pl.ds((idx % 4) * QB, QB)
        return pltpu.make_async_copy(a_hbm.at[2 * pp + p2, quarter], a_vm.at[p2, quarter], a_sem.at[idx])

    load_c = pltpu.make_async_copy(c_hbm, c_vm, c_sem)
    load_c.start()
    for idx in range(8):
        load(0, idx).start()

    barrier = pltpu.get_barrier_semaphore()

    @pl.loop(1, DEV)
    def _(k):
        pl.semaphore_signal(barrier, inc=1, device_id=(frag, (me + k) % DEV), device_id_type=MESH)

    load_c.wait()
    c = c_vm[...]
    j_row = iota((N, N), 0)
    pick_j = onehot(iota((N, N), 1) == 2 * COLS * chip_of(j_row // (2 * COLS)) + j_row % (2 * COLS))
    ct_ref[...] = dot(pick_j, c, ((1,), (1,))).astype(jnp.bfloat16)
    stacked = dot(onehot(iota((256, N), 0) % 128 == iota((256, N), 1)), c).astype(jnp.bfloat16)
    both = dot(stacked, onehot(iota((N, 256), 1) % 128 == iota((N, 256), 0)))
    c_two = jnp.where(iota((256, 256), 0) // 128 == iota((256, 256), 1) // 128, both, 0.0).astype(jnp.bfloat16)
    gap = jnp.zeros((N, 32), jnp.bfloat16)
    row = iota((2 * N, N), 0)
    pick_a = onehot(iota((2 * N, N), 1) == 8 * (row // 16) + row % 8)
    c_rows = dot(pick_a, c, ((1,), (1,))).astype(jnp.bfloat16)
    wide = dot(c_rows, onehot(iota((N, 2 * N), 1) % N == iota((N, 2 * N), 0)))
    same_p = (iota((2 * N, 2 * N), 0) % 16) // 8 == iota((2 * N, 2 * N), 1) // N
    cc_ref[...] = jnp.where(same_p, wide, 0.0).astype(jnp.bfloat16)

    lane = iota((N, 128), 1)

    def block(pp, src, tiles):
        if isinstance(pp, int) and pp == PAIRS - 1:
            return g_last.at[src, tiles]
        return g_first.at[pp, src, tiles]

    def copy_out(pp, dest, part=None):
        tiles = pl.ds(0, TILES) if part is None else pl.ds(part * PART, PART)
        return pltpu.make_async_remote_copy(
            src_ref=send.at[pp, dest, tiles],
            dst_ref=block(pp, me, tiles),
            send_sem=send_sem.at[pp, dest],
            recv_sem=recv_sem.at[pp, me],
            device_id=(frag, dest),
            device_id_type=MESH,
        )

    def wait_recv(pp, src):
        tiles = pl.ds(0, TILES)
        pltpu.make_async_remote_copy(
            src_ref=send.at[pp, src, tiles], dst_ref=block(pp, src, tiles),
            send_sem=send_sem.at[pp, src], recv_sem=recv_sem.at[pp, src],
            device_id=(frag, src), device_id_type=MESH,
        ).wait_recv()

    def half_transform(pp, first, rows, loads, wait=True):
        @pl.loop(0, 8 // loads)
        def _(step):
            if wait:
                for i in range(loads):
                    load(pp, step * loads + i).wait()
            p2, q0 = step * loads // 4, (step * loads % 4) * QB
            t_rows = []
            for i in range(0, loads * QB, 2):
                two = jnp.concatenate([a_vm[p2, q0 + i], gap, a_vm[p2, q0 + i + 1], gap], axis=1)
                t_rows.append(dot(ct_ref[first:first + rows], two).astype(jnp.bfloat16))
            half = dot(jnp.concatenate(t_rows, axis=0), c_two)
            for i in range(loads * QB):
                part = half[(i // 2) * rows:(i // 2 + 1) * rows, (i % 2) * 128:(i % 2 + 1) * 128]
                h_scr[p2, pl.ds(first * QPAD + q0 + i, rows, stride=QPAD), :] = part

    def pack(pp, slot):
        dest_chip = chip_of(slot)
        halves = []
        for p in range(2):
            tiles, last = [], []
            for cc in range(2):
                j0 = (slot * 2 + cc) * COLS
                x = [h_scr[p, pl.ds((j0 + l) * QPAD, N), :] for l in range(COLS)]
                r1, r2, r3 = pltpu.roll(x[1], 96, 1), pltpu.roll(x[2], 64, 1), pltpu.roll(x[3], 32, 1)
                r5 = pltpu.roll(x[5], 96, 1)
                tiles += [jnp.where(lane < 96, x[0], r1), jnp.where(lane < 64, r1, r2),
                          jnp.where(lane < 32, r2, r3), jnp.where(lane < 96, x[4], r5)]
                last.append(r5 if cc == 0 else pltpu.roll(x[5], 32, 1))
            tiles.append(jnp.where(lane < 64, last[0], last[1]))
            halves.append(jnp.concatenate([t.astype(jnp.bfloat16) for t in tiles], axis=1))
        out = dot(cc_ref[...], jnp.concatenate(halves, axis=0))
        for cc in range(2):
            dest = dest_chip * 2 + cc
            for t in range(4):
                tile = out[:, (cc * 4 + t) * 128:(cc * 4 + t + 1) * 128].astype(jnp.bfloat16)
                for g in range(12):
                    send[pp, dest, g * 4 + t] = tile[g * 16:(g + 1) * 16]
        low = iota((16, 128), 1) < 64
        for u in range(6):
            upper = out[u * 32:u * 32 + 16, 1024:]
            lower = out[u * 32 + 16:u * 32 + 32, 1024:]
            send[pp, dest_chip * 2, 48 + u] = jnp.where(low, upper, pltpu.roll(lower, 64, 1)).astype(jnp.bfloat16)
            send[pp, dest_chip * 2 + 1, 48 + u] = jnp.where(low, pltpu.roll(upper, 64, 1), lower).astype(jnp.bfloat16)

    def send_groups(pp, groups):
        for group in groups:
            for slot in group:
                pack(pp, slot)

            @pl.loop(0, TILES // PART)
            def _(part):
                for cc in range(2):
                    for slot in group:
                        if slot < 7:
                            copy_out(pp, chip_of(slot) * 2 + cc, part).start()
                        elif cc == 1:
                            copy_out(pp, chip * 2 + 1 - core, part).start()

    def copy_own(pp):
        return pltpu.make_async_copy(send.at[pp, me], block(pp, me, pl.ds(0, TILES)), own_sem.at[pp])

    half_transform(0, 0, HEAD, 2)
    pl.semaphore_wait(barrier, DEV - 1)
    send_groups(0, ((0, 1),))
    half_transform(0, HEAD, N - HEAD, 1, wait=False)
    for idx in range(8):
        load(1, idx).start()
    send_groups(0, FIRST_GROUPS)
    copy_own(0).start()
    for pp in range(1, PAIRS):
        half_transform(pp, 0, N, 1)
        if pp < PAIRS - 1:
            for idx in range(8):
                load(pp + 1, idx).start()
        send_groups(pp, LATER_GROUPS)
        copy_own(pp).start()

    spread = dot(onehot(iota((K8, N), 0) // 8 == iota((K8, N), 1)), c, ((1,), (1,))).astype(jnp.bfloat16)
    col, p_row = iota((N, KP), 1), iota((N, KP), 0)
    same = iota((K8, KP), 0) % 8 == iota((K8, KP), 1) % 8
    for pp in range(PAIRS):
        full = dot(spread, onehot(p_row == (col // 16) * COLS + 2 * pp + (col % 16) // 8))
        kc = jnp.where(same, full, 0.0).astype(jnp.bfloat16)
        if pp < PAIRS - 1:
            kc_first[:, pp * KP:(pp + 1) * KP] = kc
        else:
            kc_ref[...] = kc

    for pp in range(PAIRS - 1):
        copy_own(pp).wait()

        @pl.loop(1, DEV)
        def _(k):
            wait_recv(pp, (me + k) % DEV)

    def rhs_first(tile):
        return jnp.concatenate([g_first[pp, :, tile].reshape(KP, 128) for pp in range(PAIRS - 1)], axis=0)

    for third, vm_ref in enumerate((vm0_ref, vm1_ref, vm2_ref)):
        @pl.loop(0, 4)
        def _(g):
            for n in range(2):
                rhs = jnp.concatenate([rhs_first((4 * third + g) * 4 + 2 * n + t) for t in range(2)], axis=1)
                vm_ref[g, :, n * 256:(n + 1) * 256] = dot(kc_first[...], rhs)

    @pl.loop(0, 6)
    def _(u):
        vh_ref[u] = dot(kc_first[...], rhs_first(48 + u))

    for pp in range(PAIRS):
        @pl.loop(1, DEV)
        def _(k):
            copy_out(pp, (me + k) % DEV).wait_send()

    copy_own(PAIRS - 1).wait()

    @pl.loop(1, DEV)
    def _(k):
        wait_recv(PAIRS - 1, (me + k) % DEV)


def last_kernel(g_ref, vm0_ref, vm1_ref, vm2_ref, vh_ref, kc_ref, v_hbm, slots, sems):
    def put(g, slot):
        rows = pl.ds(pl.multiple_of(8 * g, 8), 8)
        return pltpu.make_async_copy(slots.at[slot], v_hbm.at[:, rows], sems.at[slot])

    for third, vm_ref in enumerate((vm0_ref, vm1_ref, vm2_ref)):
        @pl.loop(0, 2)
        def _(h):
            u = 2 * third + h
            kc = kc_ref[...]
            both = vh_ref[u] + dot(kc, g_ref[:, 48 + u].reshape(KP, 128))
            for parity in range(2):
                slot = 2 * h + parity
                g = 4 * third + slot
                if third > 0:
                    put(g - 4, slot).wait()
                for n in range(2):
                    rhs = jnp.concatenate([g_ref[:, g * 4 + 2 * n + t].reshape(KP, 128) for t in range(2)], axis=1)
                    out = vm_ref[slot, :, n * 256:(n + 1) * 256] + dot(kc, rhs)
                    slots[slot, :, :, n * 256:(n + 1) * 256] = out.reshape(N, 8, 256)
                edge = both if parity == 0 else pltpu.roll(both, 64, 1)
                slots[slot, :, :, 512:576] = edge.reshape(N, 8, 128)[:, :, :64]
                put(g, slot).start()

    for slot in range(4):
        put(8 + slot, slot).wait()


def solution(mesh):
    def local_transform(ao_rows, coeffs):
        vmem = pl.BlockSpec(memory_space=pltpu.VMEM)
        hbm = pl.BlockSpec(memory_space=pltpu.HBM)
        parts = pl.pallas_call(
            exchange_kernel,
            out_shape=(pltpu.VMEM((DEV, TILES, 16, 128), jnp.bfloat16),
                       *[pltpu.VMEM((4, K8, 512), jnp.float32)] * 3,
                       pltpu.VMEM((6, K8, 128), jnp.float32),
                       pltpu.VMEM((K8, KP), jnp.bfloat16)),
            in_specs=[hbm, hbm],
            out_specs=(vmem,) * 6,
            scratch_shapes=[
                pltpu.VMEM((2, N, N, N), jnp.bfloat16),
                pltpu.VMEM((N, N), jnp.bfloat16),
                pltpu.VMEM((N, N), jnp.bfloat16),
                pltpu.VMEM((2, N * QPAD, 128), jnp.float32),
                pltpu.VMEM((PAIRS, DEV, TILES, 16, 128), jnp.bfloat16),
                pltpu.VMEM((PAIRS - 1, DEV, TILES, 16, 128), jnp.bfloat16),
                pltpu.VMEM((2 * N, 2 * N), jnp.bfloat16),
                pltpu.VMEM((K8, (PAIRS - 1) * KP), jnp.bfloat16),
                pltpu.SemaphoreType.DMA((8,)),
                pltpu.SemaphoreType.DMA,
                pltpu.SemaphoreType.DMA((PAIRS, DEV)),
                pltpu.SemaphoreType.DMA((PAIRS, DEV)),
                pltpu.SemaphoreType.DMA((PAIRS,)),
            ],
            compiler_params=pltpu.CompilerParams(collective_id=0, has_side_effects=True, vmem_limit_bytes=34 * 2**20),
            cost_estimate=pl.CostEstimate(flops=10**10, bytes_accessed=40 * 10**6, transcendentals=0),
            name='exchange',
        )(*[pltpu.with_memory_space_constraint(x, pltpu.HBM) for x in (ao_rows, coeffs)])
        return pl.pallas_call(
            last_kernel,
            out_shape=jax.ShapeDtypeStruct((N, N, COLS * N), jnp.float32),
            in_specs=[vmem] * 6,
            out_specs=pl.BlockSpec(memory_space=pltpu.HBM),
            scratch_shapes=[pltpu.VMEM((4, N, 8, COLS * N), jnp.float32), pltpu.SemaphoreType.DMA((4,))],
            compiler_params=pltpu.CompilerParams(vmem_limit_bytes=12 * 2**20),
            cost_estimate=pl.CostEstimate(flops=3 * 10**9, bytes_accessed=24 * 10**6, transcendentals=0),
            name='last_product',
        )(*[pltpu.with_memory_space_constraint(x, pltpu.VMEM) for x in parts])

    return jax.shard_map(local_transform, mesh=mesh, in_specs=(P(('frag', 'dev')), P('frag')), out_specs=P('frag', None, 'dev'), check_vma=False)
```

```python
import jax
import jax.numpy as jnp
from jax import lax
from jax.experimental import pallas as pl
from jax.experimental.pallas import tpu as pltpu
from jax.sharding import PartitionSpec as P

MESH = pl.DeviceIdType.MESH
N = 96
DEV = 16
PAIRS = 3
COLS = 6
QPAD = 104
QB = 24
TILES = 54
PART = 9
K8 = 8 * N
KP = 16 * DEV
HEAD = 16
FIRST_GROUPS = ((1, 2, 3), (4, 5, 6, 7))
LATER_GROUPS = ((0, 3, 4, 6, 1, 2, 5, 7),)


def iota(shape, dim):
    return lax.broadcasted_iota(jnp.int32, shape, dim)


def onehot(mask):
    return jnp.where(mask, 1.0, 0.0).astype(jnp.bfloat16)


def dot(x, y, dims=((1,), (0,))):
    return lax.dot_general(x, y, (dims, ((), ())), preferred_element_type=jnp.float32)


def exchange_kernel(a_hbm, c_hbm, g_last, vm0_ref, vm1_ref, vm2_ref, vh_ref, kc_ref,
                    a_vm, c_vm, ct_ref, h_scr, send, g_first, cc_ref, kc_first, a_sem, c_sem, send_sem, recv_sem, own_sem):
    frag = lax.axis_index('frag')
    me = lax.axis_index('dev')
    chip, core = me // 2, me % 2
    cz1, cz0, cy = chip // 4, (chip // 2) % 2, chip % 2

    def chip_of(slot):
        m = 7 - slot
        return 4 * ((cz1 + m // 4) % 2) + 2 * ((cz0 + (m // 2) % 2) % 2) + (cy + m % 2) % 2

    def load(pp, idx):
        p2, quarter = idx // 4, pl.ds((idx % 4) * QB, QB)
        return pltpu.make_async_copy(a_hbm.at[2 * pp + p2, quarter], a_vm.at[p2, quarter], a_sem.at[idx])

    load_c = pltpu.make_async_copy(c_hbm, c_vm, c_sem)
    load_c.start()
    for idx in range(8):
        load(0, idx).start()

    barrier = pltpu.get_barrier_semaphore()

    @pl.loop(1, DEV)
    def _(k):
        pl.semaphore_signal(barrier, inc=1, device_id=(frag, (me + k) % DEV), device_id_type=MESH)

    load_c.wait()
    c = c_vm[...]
    j_row = iota((N, N), 0)
    pick_j = onehot(iota((N, N), 1) == 2 * COLS * chip_of(j_row // (2 * COLS)) + j_row % (2 * COLS))
    ct_ref[...] = dot(pick_j, c, ((1,), (1,))).astype(jnp.bfloat16)
    stacked = dot(onehot(iota((256, N), 0) % 128 == iota((256, N), 1)), c).astype(jnp.bfloat16)
    both = dot(stacked, onehot(iota((N, 256), 1) % 128 == iota((N, 256), 0)))
    c_two = jnp.where(iota((256, 256), 0) // 128 == iota((256, 256), 1) // 128, both, 0.0).astype(jnp.bfloat16)
    gap = jnp.zeros((N, 32), jnp.bfloat16)
    lane = iota((N, 128), 1)

    def block(pp, src, tiles):
        if isinstance(pp, int) and pp == PAIRS - 1:
            return g_last.at[src, tiles]
        return g_first.at[pp, src, tiles]

    def copy_out(pp, dest, part=None):
        tiles = pl.ds(0, TILES) if part is None else pl.ds(part * PART, PART)
        return pltpu.make_async_remote_copy(
            src_ref=send.at[pp, dest, tiles],
            dst_ref=block(pp, me, tiles),
            send_sem=send_sem.at[pp, dest],
            recv_sem=recv_sem.at[pp, me],
            device_id=(frag, dest),
            device_id_type=MESH,
        )

    def wait_recv(pp, src):
        tiles = pl.ds(0, TILES)
        pltpu.make_async_remote_copy(
            src_ref=send.at[pp, src, tiles], dst_ref=block(pp, src, tiles),
            send_sem=send_sem.at[pp, src], recv_sem=recv_sem.at[pp, src],
            device_id=(frag, src), device_id_type=MESH,
        ).wait_recv()

    def half_transform(pp, first, rows, loads, wait=True):
        @pl.loop(0, 8 // loads)
        def _(step):
            if wait:
                for i in range(loads):
                    load(pp, step * loads + i).wait()
            p2, q0 = step * loads // 4, (step * loads % 4) * QB
            t_rows = []
            for i in range(0, loads * QB, 2):
                two = jnp.concatenate([a_vm[p2, q0 + i], gap, a_vm[p2, q0 + i + 1], gap], axis=1)
                t_rows.append(dot(ct_ref[first:first + rows], two).astype(jnp.bfloat16))
            half = dot(jnp.concatenate(t_rows, axis=0), c_two)
            for i in range(loads * QB):
                part = half[(i // 2) * rows:(i // 2 + 1) * rows, (i % 2) * 128:(i % 2 + 1) * 128]
                h_scr[p2, pl.ds(first * QPAD + q0 + i, rows, stride=QPAD), :] = part

    def pack(pp, slot):
        dest_chip = chip_of(slot)
        halves = []
        for p in range(2):
            tiles, last = [], []
            for cc in range(2):
                j0 = (slot * 2 + cc) * COLS
                x = [h_scr[p, pl.ds((j0 + l) * QPAD, N), :] for l in range(COLS)]
                r1, r2, r3 = pltpu.roll(x[1], 96, 1), pltpu.roll(x[2], 64, 1), pltpu.roll(x[3], 32, 1)
                r5 = pltpu.roll(x[5], 96, 1)
                tiles += [jnp.where(lane < 96, x[0], r1), jnp.where(lane < 64, r1, r2),
                          jnp.where(lane < 32, r2, r3), jnp.where(lane < 96, x[4], r5)]
                last.append(r5 if cc == 0 else pltpu.roll(x[5], 32, 1))
            tiles.append(jnp.where(lane < 64, last[0], last[1]))
            halves.append(jnp.concatenate([t.astype(jnp.bfloat16) for t in tiles], axis=1))
        out = dot(cc_ref[...], jnp.concatenate(halves, axis=0))
        for cc in range(2):
            dest = dest_chip * 2 + cc
            for t in range(4):
                tile = out[:, (cc * 4 + t) * 128:(cc * 4 + t + 1) * 128].astype(jnp.bfloat16)
                for g in range(12):
                    send[pp, dest, g * 4 + t] = tile[g * 16:(g + 1) * 16]
        low = iota((16, 128), 1) < 64
        for u in range(6):
            upper = out[u * 32:u * 32 + 16, 1024:]
            lower = out[u * 32 + 16:u * 32 + 32, 1024:]
            send[pp, dest_chip * 2, 48 + u] = jnp.where(low, upper, pltpu.roll(lower, 64, 1)).astype(jnp.bfloat16)
            send[pp, dest_chip * 2 + 1, 48 + u] = jnp.where(low, pltpu.roll(upper, 64, 1), lower).astype(jnp.bfloat16)

    def send_groups(pp, groups):
        for group in groups:
            for slot in group:
                pack(pp, slot)

            @pl.loop(0, TILES // PART)
            def _(part):
                for turn in range(2):
                    for n, slot in enumerate(group):
                        if slot < 7:
                            copy_out(pp, chip_of(slot) * 2 + (core + turn + n) % 2, part).start()
                        elif turn == 1:
                            copy_out(pp, chip * 2 + 1 - core, part).start()

    def copy_own(pp):
        return pltpu.make_async_copy(send.at[pp, me], block(pp, me, pl.ds(0, TILES)), own_sem.at[pp])

    half_transform(0, 0, HEAD, 2)
    row = iota((2 * N, N), 0)
    pick_a = onehot(iota((2 * N, N), 1) == 8 * (row // 16) + row % 8)
    c_rows = dot(pick_a, c, ((1,), (1,))).astype(jnp.bfloat16)
    wide = dot(c_rows, onehot(iota((N, 2 * N), 1) % N == iota((N, 2 * N), 0)))
    same_p = (iota((2 * N, 2 * N), 0) % 16) // 8 == iota((2 * N, 2 * N), 1) // N
    cc_ref[...] = jnp.where(same_p, wide, 0.0).astype(jnp.bfloat16)
    pl.semaphore_wait(barrier, DEV - 1)
    send_groups(0, ((0,),))
    half_transform(0, HEAD, N - HEAD, 1, wait=False)
    for idx in range(8):
        load(1, idx).start()
    send_groups(0, FIRST_GROUPS)
    copy_own(0).start()
    for pp in range(1, PAIRS):
        half_transform(pp, 0, N, 1)
        if pp < PAIRS - 1:
            for idx in range(8):
                load(pp + 1, idx).start()
        send_groups(pp, LATER_GROUPS)
        copy_own(pp).start()

    spread = dot(onehot(iota((K8, N), 0) // 8 == iota((K8, N), 1)), c, ((1,), (1,))).astype(jnp.bfloat16)
    col, p_row = iota((N, KP), 1), iota((N, KP), 0)
    same = iota((K8, KP), 0) % 8 == iota((K8, KP), 1) % 8
    for pp in range(PAIRS):
        full = dot(spread, onehot(p_row == (col // 16) * COLS + 2 * pp + (col % 16) // 8))
        kc = jnp.where(same, full, 0.0).astype(jnp.bfloat16)
        if pp < PAIRS - 1:
            kc_first[:, pp * KP:(pp + 1) * KP] = kc
        else:
            kc_ref[...] = kc

    for pp in range(PAIRS - 1):
        copy_own(pp).wait()

        @pl.loop(1, DEV)
        def _(k):
            wait_recv(pp, (me + k) % DEV)

    def rhs_first(tile):
        return jnp.concatenate([g_first[pp, :, tile].reshape(KP, 128) for pp in range(PAIRS - 1)], axis=0)

    for third, vm_ref in enumerate((vm0_ref, vm1_ref, vm2_ref)):
        @pl.loop(0, 4)
        def _(g):
            for n in range(2):
                rhs = jnp.concatenate([rhs_first((4 * third + g) * 4 + 2 * n + t) for t in range(2)], axis=1)
                vm_ref[g, :, n * 256:(n + 1) * 256] = dot(kc_first[...], rhs)

    @pl.loop(0, 6)
    def _(u):
        vh_ref[u] = dot(kc_first[...], rhs_first(48 + u))

    for pp in range(PAIRS):
        @pl.loop(1, DEV)
        def _(k):
            copy_out(pp, (me + k) % DEV).wait_send()

    copy_own(PAIRS - 1).wait()

    @pl.loop(1, DEV)
    def _(k):
        wait_recv(PAIRS - 1, (me + k) % DEV)


def last_kernel(g_ref, vm0_ref, vm1_ref, vm2_ref, vh_ref, kc_ref, v_hbm, slots, sems):
    def put(g, slot):
        rows = pl.ds(pl.multiple_of(8 * g, 8), 8)
        return pltpu.make_async_copy(slots.at[slot], v_hbm.at[:, rows], sems.at[slot])

    for third, vm_ref in enumerate((vm0_ref, vm1_ref, vm2_ref)):
        @pl.loop(0, 2)
        def _(h):
            u = 2 * third + h
            kc = kc_ref[...]
            both = vh_ref[u] + dot(kc, g_ref[:, 48 + u].reshape(KP, 128))
            for parity in range(2):
                slot = 2 * h + parity
                g = 4 * third + slot
                if third > 0:
                    put(g - 4, slot).wait()
                for n in range(2):
                    rhs = jnp.concatenate([g_ref[:, g * 4 + 2 * n + t].reshape(KP, 128) for t in range(2)], axis=1)
                    out = vm_ref[slot, :, n * 256:(n + 1) * 256] + dot(kc, rhs)
                    slots[slot, :, :, n * 256:(n + 1) * 256] = out.reshape(N, 8, 256)
                edge = both if parity == 0 else pltpu.roll(both, 64, 1)
                slots[slot, :, :, 512:576] = edge.reshape(N, 8, 128)[:, :, :64]
                put(g, slot).start()

    for slot in range(4):
        put(8 + slot, slot).wait()


def solution(mesh):
    def local_transform(ao_rows, coeffs):
        vmem = pl.BlockSpec(memory_space=pltpu.VMEM)
        hbm = pl.BlockSpec(memory_space=pltpu.HBM)
        parts = pl.pallas_call(
            exchange_kernel,
            out_shape=(pltpu.VMEM((DEV, TILES, 16, 128), jnp.bfloat16),
                       *[pltpu.VMEM((4, K8, 512), jnp.float32)] * 3,
                       pltpu.VMEM((6, K8, 128), jnp.float32),
                       pltpu.VMEM((K8, KP), jnp.bfloat16)),
            in_specs=[hbm, hbm],
            out_specs=(vmem,) * 6,
            scratch_shapes=[
                pltpu.VMEM((2, N, N, N), jnp.bfloat16),
                pltpu.VMEM((N, N), jnp.bfloat16),
                pltpu.VMEM((N, N), jnp.bfloat16),
                pltpu.VMEM((2, N * QPAD, 128), jnp.float32),
                pltpu.VMEM((PAIRS, DEV, TILES, 16, 128), jnp.bfloat16),
                pltpu.VMEM((PAIRS - 1, DEV, TILES, 16, 128), jnp.bfloat16),
                pltpu.VMEM((2 * N, 2 * N), jnp.bfloat16),
                pltpu.VMEM((K8, (PAIRS - 1) * KP), jnp.bfloat16),
                pltpu.SemaphoreType.DMA((8,)),
                pltpu.SemaphoreType.DMA,
                pltpu.SemaphoreType.DMA((PAIRS, DEV)),
                pltpu.SemaphoreType.DMA((PAIRS, DEV)),
                pltpu.SemaphoreType.DMA((PAIRS,)),
            ],
            compiler_params=pltpu.CompilerParams(collective_id=0, has_side_effects=True, vmem_limit_bytes=34 * 2**20),
            cost_estimate=pl.CostEstimate(flops=10**10, bytes_accessed=40 * 10**6, transcendentals=0),
            name='exchange',
        )(*[pltpu.with_memory_space_constraint(x, pltpu.HBM) for x in (ao_rows, coeffs)])
        return pl.pallas_call(
            last_kernel,
            out_shape=jax.ShapeDtypeStruct((N, N, COLS * N), jnp.float32),
            in_specs=[vmem] * 6,
            out_specs=pl.BlockSpec(memory_space=pltpu.HBM),
            scratch_shapes=[pltpu.VMEM((4, N, 8, COLS * N), jnp.float32), pltpu.SemaphoreType.DMA((4,))],
            compiler_params=pltpu.CompilerParams(vmem_limit_bytes=12 * 2**20),
            cost_estimate=pl.CostEstimate(flops=3 * 10**9, bytes_accessed=24 * 10**6, transcendentals=0),
            name='last_product',
        )(*[pltpu.with_memory_space_constraint(x, pltpu.VMEM) for x in parts])

    return jax.shard_map(local_transform, mesh=mesh, in_specs=(P(('frag', 'dev')), P('frag')), out_specs=P('frag', None, 'dev'), check_vma=False)
```

```python
import jax
import jax.numpy as jnp
from jax import lax
from jax.experimental import pallas as pl
from jax.experimental.pallas import tpu as pltpu
from jax.sharding import PartitionSpec as P

MESH = pl.DeviceIdType.MESH
N = 96
DEV = 16
PAIRS = 3
COLS = 6
QPAD = 104
QB = 24
TILES = 54
PART = 9
K8 = 8 * N
KP = 16 * DEV
HEAD = 16
FIRST_GROUPS = ((3, 4, 6, 1, 2, 5, 7),)
LATER_GROUPS = ((0, 3, 4, 6, 1, 2, 5, 7),)


def iota(shape, dim):
    return lax.broadcasted_iota(jnp.int32, shape, dim)


def onehot(mask):
    return jnp.where(mask, 1.0, 0.0).astype(jnp.bfloat16)


def dot(x, y, dims=((1,), (0,))):
    return lax.dot_general(x, y, (dims, ((), ())), preferred_element_type=jnp.float32)


def exchange_kernel(a_hbm, c_hbm, g_last, vm0_ref, vm1_ref, vm2_ref, vh_ref, kc_ref,
                    a_vm, c_vm, ct_ref, h_scr, send, g_first, cc_ref, kc_first, a_sem, c_sem, send_sem, recv_sem, own_sem):
    frag = lax.axis_index('frag')
    me = lax.axis_index('dev')
    chip, core = me // 2, me % 2
    cz1, cz0, cy = chip // 4, (chip // 2) % 2, chip % 2

    def chip_of(slot):
        m = 7 - slot
        return 4 * ((cz1 + m // 4) % 2) + 2 * ((cz0 + (m // 2) % 2) % 2) + (cy + m % 2) % 2

    def load(pp, idx):
        p2, quarter = idx // 4, pl.ds((idx % 4) * QB, QB)
        return pltpu.make_async_copy(a_hbm.at[2 * pp + p2, quarter], a_vm.at[p2, quarter], a_sem.at[idx])

    load_c = pltpu.make_async_copy(c_hbm, c_vm, c_sem)
    load_c.start()
    for idx in range(8):
        load(0, idx).start()

    barrier = pltpu.get_barrier_semaphore()

    @pl.loop(1, DEV)
    def _(k):
        pl.semaphore_signal(barrier, inc=1, device_id=(frag, (me + k) % DEV), device_id_type=MESH)

    load_c.wait()
    c = c_vm[...]
    j_row = iota((N, N), 0)
    pick_j = onehot(iota((N, N), 1) == 2 * COLS * chip_of(j_row // (2 * COLS)) + j_row % (2 * COLS))
    ct_ref[...] = dot(pick_j, c, ((1,), (1,))).astype(jnp.bfloat16)
    stacked = dot(onehot(iota((256, N), 0) % 128 == iota((256, N), 1)), c).astype(jnp.bfloat16)
    both = dot(stacked, onehot(iota((N, 256), 1) % 128 == iota((N, 256), 0)))
    c_two = jnp.where(iota((256, 256), 0) // 128 == iota((256, 256), 1) // 128, both, 0.0).astype(jnp.bfloat16)
    gap = jnp.zeros((N, 32), jnp.bfloat16)
    lane = iota((N, 128), 1)

    def block(pp, src, tiles):
        if isinstance(pp, int) and pp == PAIRS - 1:
            return g_last.at[src, tiles]
        return g_first.at[pp, src, tiles]

    def copy_out(pp, dest, part=None):
        tiles = pl.ds(0, TILES) if part is None else pl.ds(part * PART, PART)
        return pltpu.make_async_remote_copy(
            src_ref=send.at[pp, dest, tiles],
            dst_ref=block(pp, me, tiles),
            send_sem=send_sem.at[pp, dest],
            recv_sem=recv_sem.at[pp, me],
            device_id=(frag, dest),
            device_id_type=MESH,
        )

    def wait_recv(pp, src):
        tiles = pl.ds(0, TILES)
        pltpu.make_async_remote_copy(
            src_ref=send.at[pp, src, tiles], dst_ref=block(pp, src, tiles),
            send_sem=send_sem.at[pp, src], recv_sem=recv_sem.at[pp, src],
            device_id=(frag, src), device_id_type=MESH,
        ).wait_recv()

    def half_transform(pp, first, rows, loads, wait=True):
        @pl.loop(0, 8 // loads)
        def _(step):
            if wait:
                for i in range(loads):
                    load(pp, step * loads + i).wait()
            p2, q0 = step * loads // 4, (step * loads % 4) * QB
            t_rows = []
            for i in range(0, loads * QB, 2):
                two = jnp.concatenate([a_vm[p2, q0 + i], gap, a_vm[p2, q0 + i + 1], gap], axis=1)
                t_rows.append(dot(ct_ref[first:first + rows], two).astype(jnp.bfloat16))
            half = dot(jnp.concatenate(t_rows, axis=0), c_two)
            for i in range(loads * QB):
                part = half[(i // 2) * rows:(i // 2 + 1) * rows, (i % 2) * 128:(i % 2 + 1) * 128]
                h_scr[p2, pl.ds(first * QPAD + q0 + i, rows, stride=QPAD), :] = part

    def pack(pp, slot):
        dest_chip = chip_of(slot)
        halves = []
        for p in range(2):
            tiles, last = [], []
            for cc in range(2):
                j0 = (slot * 2 + cc) * COLS
                x = [h_scr[p, pl.ds((j0 + l) * QPAD, N), :] for l in range(COLS)]
                r1, r2, r3 = pltpu.roll(x[1], 96, 1), pltpu.roll(x[2], 64, 1), pltpu.roll(x[3], 32, 1)
                r5 = pltpu.roll(x[5], 96, 1)
                tiles += [jnp.where(lane < 96, x[0], r1), jnp.where(lane < 64, r1, r2),
                          jnp.where(lane < 32, r2, r3), jnp.where(lane < 96, x[4], r5)]
                last.append(r5 if cc == 0 else pltpu.roll(x[5], 32, 1))
            tiles.append(jnp.where(lane < 64, last[0], last[1]))
            halves.append(jnp.concatenate([t.astype(jnp.bfloat16) for t in tiles], axis=1))
        out = dot(cc_ref[...], jnp.concatenate(halves, axis=0))
        for cc in range(2):
            dest = dest_chip * 2 + cc
            for t in range(4):
                tile = out[:, (cc * 4 + t) * 128:(cc * 4 + t + 1) * 128].astype(jnp.bfloat16)
                for g in range(12):
                    send[pp, dest, g * 4 + t] = tile[g * 16:(g + 1) * 16]
        low = iota((16, 128), 1) < 64
        for u in range(6):
            upper = out[u * 32:u * 32 + 16, 1024:]
            lower = out[u * 32 + 16:u * 32 + 32, 1024:]
            send[pp, dest_chip * 2, 48 + u] = jnp.where(low, upper, pltpu.roll(lower, 64, 1)).astype(jnp.bfloat16)
            send[pp, dest_chip * 2 + 1, 48 + u] = jnp.where(low, pltpu.roll(upper, 64, 1), lower).astype(jnp.bfloat16)

    def send_groups(pp, groups):
        for group in groups:
            for slot in group:
                pack(pp, slot)

            @pl.loop(0, TILES // PART)
            def _(part):
                for turn in range(2):
                    for slot in group:
                        if slot < 7:
                            copy_out(pp, chip_of(slot) * 2 + turn, part).start()
                        elif turn == 1:
                            copy_out(pp, chip * 2 + 1 - core, part).start()

    def copy_own(pp):
        return pltpu.make_async_copy(send.at[pp, me], block(pp, me, pl.ds(0, TILES)), own_sem.at[pp])

    half_transform(0, 0, HEAD, 2)
    row = iota((2 * N, N), 0)
    pick_a = onehot(iota((2 * N, N), 1) == 8 * (row // 16) + row % 8)
    c_rows = dot(pick_a, c, ((1,), (1,))).astype(jnp.bfloat16)
    wide = dot(c_rows, onehot(iota((N, 2 * N), 1) % N == iota((N, 2 * N), 0)))
    same_p = (iota((2 * N, 2 * N), 0) % 16) // 8 == iota((2 * N, 2 * N), 1) // N
    cc_ref[...] = jnp.where(same_p, wide, 0.0).astype(jnp.bfloat16)
    pl.semaphore_wait(barrier, DEV - 1)
    send_groups(0, ((0,),))
    half_transform(0, HEAD, N - HEAD, 1, wait=False)
    for idx in range(8):
        load(1, idx).start()
    send_groups(0, FIRST_GROUPS)
    copy_own(0).start()
    for pp in range(1, PAIRS):
        half_transform(pp, 0, N, 1)
        if pp < PAIRS - 1:
            for idx in range(8):
                load(pp + 1, idx).start()
        send_groups(pp, LATER_GROUPS)
        copy_own(pp).start()

    spread = dot(onehot(iota((K8, N), 0) // 8 == iota((K8, N), 1)), c, ((1,), (1,))).astype(jnp.bfloat16)
    col, p_row = iota((N, KP), 1), iota((N, KP), 0)
    same = iota((K8, KP), 0) % 8 == iota((K8, KP), 1) % 8
    for pp in range(PAIRS):
        full = dot(spread, onehot(p_row == (col // 16) * COLS + 2 * pp + (col % 16) // 8))
        kc = jnp.where(same, full, 0.0).astype(jnp.bfloat16)
        if pp < PAIRS - 1:
            kc_first[:, pp * KP:(pp + 1) * KP] = kc
        else:
            kc_ref[...] = kc

    for pp in range(PAIRS - 1):
        copy_own(pp).wait()

        @pl.loop(1, DEV)
        def _(k):
            wait_recv(pp, (me + k) % DEV)

    def rhs_first(tile):
        return jnp.concatenate([g_first[pp, :, tile].reshape(KP, 128) for pp in range(PAIRS - 1)], axis=0)

    for third, vm_ref in enumerate((vm0_ref, vm1_ref, vm2_ref)):
        @pl.loop(0, 4)
        def _(g):
            for n in range(2):
                rhs = jnp.concatenate([rhs_first((4 * third + g) * 4 + 2 * n + t) for t in range(2)], axis=1)
                vm_ref[g, :, n * 256:(n + 1) * 256] = dot(kc_first[...], rhs)

    @pl.loop(0, 6)
    def _(u):
        vh_ref[u] = dot(kc_first[...], rhs_first(48 + u))

    for pp in range(PAIRS):
        @pl.loop(1, DEV)
        def _(k):
            copy_out(pp, (me + k) % DEV).wait_send()

    copy_own(PAIRS - 1).wait()

    @pl.loop(1, DEV)
    def _(k):
        wait_recv(PAIRS - 1, (me + k) % DEV)


def last_kernel(g_ref, vm0_ref, vm1_ref, vm2_ref, vh_ref, kc_ref, v_hbm, slots, sems):
    def put(g, slot):
        rows = pl.ds(pl.multiple_of(8 * g, 8), 8)
        return pltpu.make_async_copy(slots.at[slot], v_hbm.at[:, rows], sems.at[slot])

    for third, vm_ref in enumerate((vm0_ref, vm1_ref, vm2_ref)):
        @pl.loop(0, 2)
        def _(h):
            u = 2 * third + h
            kc = kc_ref[...]
            both = vh_ref[u] + dot(kc, g_ref[:, 48 + u].reshape(KP, 128))
            for parity in range(2):
                slot = 2 * h + parity
                g = 4 * third + slot
                if third > 0:
                    put(g - 4, slot).wait()
                for n in range(2):
                    rhs = jnp.concatenate([g_ref[:, g * 4 + 2 * n + t].reshape(KP, 128) for t in range(2)], axis=1)
                    out = vm_ref[slot, :, n * 256:(n + 1) * 256] + dot(kc, rhs)
                    slots[slot, :, :, n * 256:(n + 1) * 256] = out.reshape(N, 8, 256)
                edge = both if parity == 0 else pltpu.roll(both, 64, 1)
                slots[slot, :, :, 512:576] = edge.reshape(N, 8, 128)[:, :, :64]
                put(g, slot).start()

    for slot in range(4):
        put(8 + slot, slot).wait()


def solution(mesh):
    def local_transform(ao_rows, coeffs):
        vmem = pl.BlockSpec(memory_space=pltpu.VMEM)
        hbm = pl.BlockSpec(memory_space=pltpu.HBM)
        parts = pl.pallas_call(
            exchange_kernel,
            out_shape=(pltpu.VMEM((DEV, TILES, 16, 128), jnp.bfloat16),
                       *[pltpu.VMEM((4, K8, 512), jnp.float32)] * 3,
                       pltpu.VMEM((6, K8, 128), jnp.float32),
                       pltpu.VMEM((K8, KP), jnp.bfloat16)),
            in_specs=[hbm, hbm],
            out_specs=(vmem,) * 6,
            scratch_shapes=[
                pltpu.VMEM((2, N, N, N), jnp.bfloat16),
                pltpu.VMEM((N, N), jnp.bfloat16),
                pltpu.VMEM((N, N), jnp.bfloat16),
                pltpu.VMEM((2, N * QPAD, 128), jnp.float32),
                pltpu.VMEM((PAIRS, DEV, TILES, 16, 128), jnp.bfloat16),
                pltpu.VMEM((PAIRS - 1, DEV, TILES, 16, 128), jnp.bfloat16),
                pltpu.VMEM((2 * N, 2 * N), jnp.bfloat16),
                pltpu.VMEM((K8, (PAIRS - 1) * KP), jnp.bfloat16),
                pltpu.SemaphoreType.DMA((8,)),
                pltpu.SemaphoreType.DMA,
                pltpu.SemaphoreType.DMA((PAIRS, DEV)),
                pltpu.SemaphoreType.DMA((PAIRS, DEV)),
                pltpu.SemaphoreType.DMA((PAIRS,)),
            ],
            compiler_params=pltpu.CompilerParams(collective_id=0, has_side_effects=True, vmem_limit_bytes=34 * 2**20),
            cost_estimate=pl.CostEstimate(flops=10**10, bytes_accessed=40 * 10**6, transcendentals=0),
            name='exchange',
        )(*[pltpu.with_memory_space_constraint(x, pltpu.HBM) for x in (ao_rows, coeffs)])
        return pl.pallas_call(
            last_kernel,
            out_shape=jax.ShapeDtypeStruct((N, N, COLS * N), jnp.float32),
            in_specs=[vmem] * 6,
            out_specs=pl.BlockSpec(memory_space=pltpu.HBM),
            scratch_shapes=[pltpu.VMEM((4, N, 8, COLS * N), jnp.float32), pltpu.SemaphoreType.DMA((4,))],
            compiler_params=pltpu.CompilerParams(vmem_limit_bytes=12 * 2**20),
            cost_estimate=pl.CostEstimate(flops=3 * 10**9, bytes_accessed=24 * 10**6, transcendentals=0),
            name='last_product',
        )(*[pltpu.with_memory_space_constraint(x, pltpu.VMEM) for x in parts])

    return jax.shard_map(local_transform, mesh=mesh, in_specs=(P(('frag', 'dev')), P('frag')), out_specs=P('frag', None, 'dev'), check_vma=False)
```

```python
import jax
import jax.numpy as jnp
from jax import lax
from jax.experimental import pallas as pl
from jax.experimental.pallas import tpu as pltpu
from jax.sharding import PartitionSpec as P

MESH = pl.DeviceIdType.MESH
N = 96
DEV = 16
PAIRS = 3
COLS = 6
QPAD = 104
QB = 24
TILES = 54
PARTS = (9, 3, 3)
K8 = 8 * N
KP = 16 * DEV
HEAD = 32
FIRST_GROUPS = ((2, 3), (4, 5, 6, 7))
LATER_GROUPS = ((0, 3, 4, 6, 1, 2, 5, 7),)


def iota(shape, dim):
    return lax.broadcasted_iota(jnp.int32, shape, dim)


def onehot(mask):
    return jnp.where(mask, 1.0, 0.0).astype(jnp.bfloat16)


def dot(x, y, dims=((1,), (0,))):
    return lax.dot_general(x, y, (dims, ((), ())), preferred_element_type=jnp.float32)


def exchange_kernel(a_hbm, c_hbm, g_last, vm0_ref, vm1_ref, vm2_ref, vh_ref, kc_ref,
                    a_vm, c_vm, ct_ref, h_scr, send, g_first, cc_ref, kc_first, a_sem, c_sem, send_sem, recv_sem, own_sem):
    frag = lax.axis_index('frag')
    me = lax.axis_index('dev')
    chip, core = me // 2, me % 2
    cz1, cz0, cy = chip // 4, (chip // 2) % 2, chip % 2

    def chip_of(slot):
        m = 7 - slot
        return 4 * ((cz1 + m // 4) % 2) + 2 * ((cz0 + (m // 2) % 2) % 2) + (cy + m % 2) % 2

    def load(pp, idx):
        p2, quarter = idx // 4, pl.ds((idx % 4) * QB, QB)
        return pltpu.make_async_copy(a_hbm.at[2 * pp + p2, quarter], a_vm.at[p2, quarter], a_sem.at[idx])

    load_c = pltpu.make_async_copy(c_hbm, c_vm, c_sem)
    load_c.start()
    for idx in range(8):
        load(0, idx).start()

    barrier = pltpu.get_barrier_semaphore()

    @pl.loop(1, DEV)
    def _(k):
        pl.semaphore_signal(barrier, inc=1, device_id=(frag, (me + k) % DEV), device_id_type=MESH)

    load_c.wait()
    c = c_vm[...]
    j_row = iota((N, N), 0)
    pick_j = onehot(iota((N, N), 1) == 2 * COLS * chip_of(j_row // (2 * COLS)) + j_row % (2 * COLS))
    ct_ref[...] = dot(pick_j, c, ((1,), (1,))).astype(jnp.bfloat16)
    stacked = dot(onehot(iota((256, N), 0) % 128 == iota((256, N), 1)), c).astype(jnp.bfloat16)
    both = dot(stacked, onehot(iota((N, 256), 1) % 128 == iota((N, 256), 0)))
    c_two = jnp.where(iota((256, 256), 0) // 128 == iota((256, 256), 1) // 128, both, 0.0).astype(jnp.bfloat16)
    gap = jnp.zeros((N, 32), jnp.bfloat16)
    lane = iota((N, 128), 1)

    def block(pp, src, tiles):
        if isinstance(pp, int) and pp == PAIRS - 1:
            return g_last.at[src, tiles]
        return g_first.at[pp, src, tiles]

    def copy_out(pp, dest, part=None):
        tiles = pl.ds(0, TILES) if part is None else pl.ds(part * PARTS[pp], PARTS[pp])
        return pltpu.make_async_remote_copy(
            src_ref=send.at[pp, dest, tiles],
            dst_ref=block(pp, me, tiles),
            send_sem=send_sem.at[pp, dest],
            recv_sem=recv_sem.at[pp, me],
            device_id=(frag, dest),
            device_id_type=MESH,
        )

    def wait_recv(pp, src):
        tiles = pl.ds(0, TILES)
        pltpu.make_async_remote_copy(
            src_ref=send.at[pp, src, tiles], dst_ref=block(pp, src, tiles),
            send_sem=send_sem.at[pp, src], recv_sem=recv_sem.at[pp, src],
            device_id=(frag, src), device_id_type=MESH,
        ).wait_recv()

    def half_transform(pp, first, rows, loads, wait=True):
        @pl.loop(0, 8 // loads)
        def _(step):
            if wait:
                for i in range(loads):
                    load(pp, step * loads + i).wait()
            p2, q0 = step * loads // 4, (step * loads % 4) * QB
            t_rows = []
            for i in range(0, loads * QB, 2):
                two = jnp.concatenate([a_vm[p2, q0 + i], gap, a_vm[p2, q0 + i + 1], gap], axis=1)
                t_rows.append(dot(ct_ref[first:first + rows], two).astype(jnp.bfloat16))
            half = dot(jnp.concatenate(t_rows, axis=0), c_two)
            for i in range(loads * QB):
                part = half[(i // 2) * rows:(i // 2 + 1) * rows, (i % 2) * 128:(i % 2 + 1) * 128]
                h_scr[p2, pl.ds(first * QPAD + q0 + i, rows, stride=QPAD), :] = part

    def pack(pp, slot):
        dest_chip = chip_of(slot)
        halves = []
        for p in range(2):
            tiles, last = [], []
            for cc in range(2):
                j0 = (slot * 2 + cc) * COLS
                x = [h_scr[p, pl.ds((j0 + l) * QPAD, N), :] for l in range(COLS)]
                r1, r2, r3 = pltpu.roll(x[1], 96, 1), pltpu.roll(x[2], 64, 1), pltpu.roll(x[3], 32, 1)
                r5 = pltpu.roll(x[5], 96, 1)
                tiles += [jnp.where(lane < 96, x[0], r1), jnp.where(lane < 64, r1, r2),
                          jnp.where(lane < 32, r2, r3), jnp.where(lane < 96, x[4], r5)]
                last.append(r5 if cc == 0 else pltpu.roll(x[5], 32, 1))
            tiles.append(jnp.where(lane < 64, last[0], last[1]))
            halves.append(jnp.concatenate([t.astype(jnp.bfloat16) for t in tiles], axis=1))
        out = dot(cc_ref[...], jnp.concatenate(halves, axis=0))
        for cc in range(2):
            dest = dest_chip * 2 + cc
            for t in range(4):
                tile = out[:, (cc * 4 + t) * 128:(cc * 4 + t + 1) * 128].astype(jnp.bfloat16)
                for g in range(12):
                    send[pp, dest, g * 4 + t] = tile[g * 16:(g + 1) * 16]
        low = iota((16, 128), 1) < 64
        for u in range(6):
            upper = out[u * 32:u * 32 + 16, 1024:]
            lower = out[u * 32 + 16:u * 32 + 32, 1024:]
            send[pp, dest_chip * 2, 48 + u] = jnp.where(low, upper, pltpu.roll(lower, 64, 1)).astype(jnp.bfloat16)
            send[pp, dest_chip * 2 + 1, 48 + u] = jnp.where(low, pltpu.roll(upper, 64, 1), lower).astype(jnp.bfloat16)

    def send_groups(pp, groups):
        for group in groups:
            for slot in group:
                pack(pp, slot)

            @pl.loop(0, TILES // PARTS[pp])
            def _(part):
                for cc in range(2):
                    for slot in group:
                        if slot < 7:
                            copy_out(pp, chip_of(slot) * 2 + cc, part).start()
                        elif cc == 1:
                            copy_out(pp, chip * 2 + 1 - core, part).start()

    def copy_own(pp):
        return pltpu.make_async_copy(send.at[pp, me], block(pp, me, pl.ds(0, TILES)), own_sem.at[pp])

    half_transform(0, 0, HEAD, 2)
    row = iota((2 * N, N), 0)
    pick_a = onehot(iota((2 * N, N), 1) == 8 * (row // 16) + row % 8)
    c_rows = dot(pick_a, c, ((1,), (1,))).astype(jnp.bfloat16)
    wide = dot(c_rows, onehot(iota((N, 2 * N), 1) % N == iota((N, 2 * N), 0)))
    same_p = (iota((2 * N, 2 * N), 0) % 16) // 8 == iota((2 * N, 2 * N), 1) // N
    cc_ref[...] = jnp.where(same_p, wide, 0.0).astype(jnp.bfloat16)
    pl.semaphore_wait(barrier, DEV - 1)
    send_groups(0, ((0, 1),))
    half_transform(0, HEAD, N - HEAD, 1, wait=False)
    for idx in range(8):
        load(1, idx).start()
    send_groups(0, FIRST_GROUPS)
    copy_own(0).start()
    for pp in range(1, PAIRS):
        half_transform(pp, 0, N, 1)
        if pp < PAIRS - 1:
            for idx in range(8):
                load(pp + 1, idx).start()
        send_groups(pp, LATER_GROUPS)
        copy_own(pp).start()

    spread = dot(onehot(iota((K8, N), 0) // 8 == iota((K8, N), 1)), c, ((1,), (1,))).astype(jnp.bfloat16)
    col, p_row = iota((N, KP), 1), iota((N, KP), 0)
    same = iota((K8, KP), 0) % 8 == iota((K8, KP), 1) % 8
    for pp in range(PAIRS):
        full = dot(spread, onehot(p_row == (col // 16) * COLS + 2 * pp + (col % 16) // 8))
        kc = jnp.where(same, full, 0.0).astype(jnp.bfloat16)
        if pp < PAIRS - 1:
            kc_first[:, pp * KP:(pp + 1) * KP] = kc
        else:
            kc_ref[...] = kc

    for pp in range(PAIRS - 1):
        copy_own(pp).wait()

        @pl.loop(1, DEV)
        def _(k):
            wait_recv(pp, (me + k) % DEV)

    def rhs_first(tile):
        return jnp.concatenate([g_first[pp, :, tile].reshape(KP, 128) for pp in range(PAIRS - 1)], axis=0)

    for third, vm_ref in enumerate((vm0_ref, vm1_ref, vm2_ref)):
        @pl.loop(0, 4)
        def _(g):
            for n in range(2):
                rhs = jnp.concatenate([rhs_first((4 * third + g) * 4 + 2 * n + t) for t in range(2)], axis=1)
                vm_ref[g, :, n * 256:(n + 1) * 256] = dot(kc_first[...], rhs)

    @pl.loop(0, 6)
    def _(u):
        vh_ref[u] = dot(kc_first[...], rhs_first(48 + u))

    for pp in range(PAIRS):
        @pl.loop(1, DEV)
        def _(k):
            copy_out(pp, (me + k) % DEV).wait_send()

    copy_own(PAIRS - 1).wait()

    @pl.loop(1, DEV)
    def _(k):
        wait_recv(PAIRS - 1, (me + k) % DEV)


def last_kernel(g_ref, vm0_ref, vm1_ref, vm2_ref, vh_ref, kc_ref, v_hbm, slots, sems):
    def put(g, slot):
        rows = pl.ds(pl.multiple_of(8 * g, 8), 8)
        return pltpu.make_async_copy(slots.at[slot], v_hbm.at[:, rows], sems.at[slot])

    for third, vm_ref in enumerate((vm0_ref, vm1_ref, vm2_ref)):
        @pl.loop(0, 2)
        def _(h):
            u = 2 * third + h
            kc = kc_ref[...]
            both = vh_ref[u] + dot(kc, g_ref[:, 48 + u].reshape(KP, 128))
            for parity in range(2):
                slot = 2 * h + parity
                g = 4 * third + slot
                if third > 0:
                    put(g - 4, slot).wait()
                for n in range(2):
                    rhs = jnp.concatenate([g_ref[:, g * 4 + 2 * n + t].reshape(KP, 128) for t in range(2)], axis=1)
                    out = vm_ref[slot, :, n * 256:(n + 1) * 256] + dot(kc, rhs)
                    slots[slot, :, :, n * 256:(n + 1) * 256] = out.reshape(N, 8, 256)
                edge = both if parity == 0 else pltpu.roll(both, 64, 1)
                slots[slot, :, :, 512:576] = edge.reshape(N, 8, 128)[:, :, :64]
                put(g, slot).start()

    for slot in range(4):
        put(8 + slot, slot).wait()


def solution(mesh):
    def local_transform(ao_rows, coeffs):
        vmem = pl.BlockSpec(memory_space=pltpu.VMEM)
        hbm = pl.BlockSpec(memory_space=pltpu.HBM)
        parts = pl.pallas_call(
            exchange_kernel,
            out_shape=(pltpu.VMEM((DEV, TILES, 16, 128), jnp.bfloat16),
                       *[pltpu.VMEM((4, K8, 512), jnp.float32)] * 3,
                       pltpu.VMEM((6, K8, 128), jnp.float32),
                       pltpu.VMEM((K8, KP), jnp.bfloat16)),
            in_specs=[hbm, hbm],
            out_specs=(vmem,) * 6,
            scratch_shapes=[
                pltpu.VMEM((2, N, N, N), jnp.bfloat16),
                pltpu.VMEM((N, N), jnp.bfloat16),
                pltpu.VMEM((N, N), jnp.bfloat16),
                pltpu.VMEM((2, N * QPAD, 128), jnp.float32),
                pltpu.VMEM((PAIRS, DEV, TILES, 16, 128), jnp.bfloat16),
                pltpu.VMEM((PAIRS - 1, DEV, TILES, 16, 128), jnp.bfloat16),
                pltpu.VMEM((2 * N, 2 * N), jnp.bfloat16),
                pltpu.VMEM((K8, (PAIRS - 1) * KP), jnp.bfloat16),
                pltpu.SemaphoreType.DMA((8,)),
                pltpu.SemaphoreType.DMA,
                pltpu.SemaphoreType.DMA((PAIRS, DEV)),
                pltpu.SemaphoreType.DMA((PAIRS, DEV)),
                pltpu.SemaphoreType.DMA((PAIRS,)),
            ],
            compiler_params=pltpu.CompilerParams(collective_id=0, has_side_effects=True, vmem_limit_bytes=34 * 2**20),
            cost_estimate=pl.CostEstimate(flops=10**10, bytes_accessed=40 * 10**6, transcendentals=0),
            name='exchange',
        )(*[pltpu.with_memory_space_constraint(x, pltpu.HBM) for x in (ao_rows, coeffs)])
        return pl.pallas_call(
            last_kernel,
            out_shape=jax.ShapeDtypeStruct((N, N, COLS * N), jnp.float32),
            in_specs=[vmem] * 6,
            out_specs=pl.BlockSpec(memory_space=pltpu.HBM),
            scratch_shapes=[pltpu.VMEM((4, N, 8, COLS * N), jnp.float32), pltpu.SemaphoreType.DMA((4,))],
            compiler_params=pltpu.CompilerParams(vmem_limit_bytes=12 * 2**20),
            cost_estimate=pl.CostEstimate(flops=3 * 10**9, bytes_accessed=24 * 10**6, transcendentals=0),
            name='last_product',
        )(*[pltpu.with_memory_space_constraint(x, pltpu.VMEM) for x in parts])

    return jax.shard_map(local_transform, mesh=mesh, in_specs=(P(('frag', 'dev')), P('frag')), out_specs=P('frag', None, 'dev'), check_vma=False)
```

```python
import jax
import jax.numpy as jnp
from jax import lax
from jax.experimental import pallas as pl
from jax.experimental.pallas import tpu as pltpu
from jax.sharding import PartitionSpec as P

MESH = pl.DeviceIdType.MESH
N = 96
DEV = 16
PAIRS = 3
COLS = 6
QPAD = 104
QB = 24
TILES = 54
PARTS = (18, 18, 9)
K8 = 8 * N
KP = 16 * DEV
HEAD = 32
FIRST_GROUPS = ((2, 3), (4, 5, 6, 7))
LATER_GROUPS = ((0, 3, 4, 6, 1, 2, 5, 7),)


def iota(shape, dim):
    return lax.broadcasted_iota(jnp.int32, shape, dim)


def onehot(mask):
    return jnp.where(mask, 1.0, 0.0).astype(jnp.bfloat16)


def dot(x, y, dims=((1,), (0,))):
    return lax.dot_general(x, y, (dims, ((), ())), preferred_element_type=jnp.float32)


def exchange_kernel(a_hbm, c_hbm, g_last, vm0_ref, vm1_ref, vm2_ref, vh_ref, kc_ref,
                    a_vm, c_vm, ct_ref, h_scr, send, g_first, cc_ref, kc_first, a_sem, c_sem, send_sem, recv_sem, own_sem):
    frag = lax.axis_index('frag')
    me = lax.axis_index('dev')
    chip, core = me // 2, me % 2
    cz1, cz0, cy = chip // 4, (chip // 2) % 2, chip % 2

    def chip_of(slot):
        m = 7 - slot
        return 4 * ((cz1 + m // 4) % 2) + 2 * ((cz0 + (m // 2) % 2) % 2) + (cy + m % 2) % 2

    def load(pp, idx):
        p2, quarter = idx // 4, pl.ds((idx % 4) * QB, QB)
        return pltpu.make_async_copy(a_hbm.at[2 * pp + p2, quarter], a_vm.at[p2, quarter], a_sem.at[idx])

    load_c = pltpu.make_async_copy(c_hbm, c_vm, c_sem)
    load_c.start()
    for idx in range(8):
        load(0, idx).start()

    barrier = pltpu.get_barrier_semaphore()

    @pl.loop(1, DEV)
    def _(k):
        pl.semaphore_signal(barrier, inc=1, device_id=(frag, (me + k) % DEV), device_id_type=MESH)

    load_c.wait()
    c = c_vm[...]
    j_row = iota((N, N), 0)
    pick_j = onehot(iota((N, N), 1) == 2 * COLS * chip_of(j_row // (2 * COLS)) + j_row % (2 * COLS))
    ct_ref[...] = dot(pick_j, c, ((1,), (1,))).astype(jnp.bfloat16)
    stacked = dot(onehot(iota((256, N), 0) % 128 == iota((256, N), 1)), c).astype(jnp.bfloat16)
    both = dot(stacked, onehot(iota((N, 256), 1) % 128 == iota((N, 256), 0)))
    c_two = jnp.where(iota((256, 256), 0) // 128 == iota((256, 256), 1) // 128, both, 0.0).astype(jnp.bfloat16)
    gap = jnp.zeros((N, 32), jnp.bfloat16)
    lane = iota((N, 128), 1)

    def block(pp, src, tiles):
        if isinstance(pp, int) and pp == PAIRS - 1:
            return g_last.at[src, tiles]
        return g_first.at[pp, src, tiles]

    def copy_out(pp, dest, part=None):
        tiles = pl.ds(0, TILES) if part is None else pl.ds(part * PARTS[pp], PARTS[pp])
        return pltpu.make_async_remote_copy(
            src_ref=send.at[pp, dest, tiles],
            dst_ref=block(pp, me, tiles),
            send_sem=send_sem.at[pp, dest],
            recv_sem=recv_sem.at[pp, me],
            device_id=(frag, dest),
            device_id_type=MESH,
        )

    def wait_recv(pp, src):
        tiles = pl.ds(0, TILES)
        pltpu.make_async_remote_copy(
            src_ref=send.at[pp, src, tiles], dst_ref=block(pp, src, tiles),
            send_sem=send_sem.at[pp, src], recv_sem=recv_sem.at[pp, src],
            device_id=(frag, src), device_id_type=MESH,
        ).wait_recv()

    def half_transform(pp, first, rows, loads, wait=True):
        @pl.loop(0, 8 // loads)
        def _(step):
            if wait:
                for i in range(loads):
                    load(pp, step * loads + i).wait()
            p2, q0 = step * loads // 4, (step * loads % 4) * QB
            t_rows = []
            for i in range(0, loads * QB, 2):
                two = jnp.concatenate([a_vm[p2, q0 + i], gap, a_vm[p2, q0 + i + 1], gap], axis=1)
                t_rows.append(dot(ct_ref[first:first + rows], two).astype(jnp.bfloat16))
            half = dot(jnp.concatenate(t_rows, axis=0), c_two)
            for i in range(loads * QB):
                part = half[(i // 2) * rows:(i // 2 + 1) * rows, (i % 2) * 128:(i % 2 + 1) * 128]
                h_scr[p2, pl.ds(first * QPAD + q0 + i, rows, stride=QPAD), :] = part

    def pack(pp, slot):
        dest_chip = chip_of(slot)
        halves = []
        for p in range(2):
            tiles, last = [], []
            for cc in range(2):
                j0 = (slot * 2 + cc) * COLS
                x = [h_scr[p, pl.ds((j0 + l) * QPAD, N), :] for l in range(COLS)]
                r1, r2, r3 = pltpu.roll(x[1], 96, 1), pltpu.roll(x[2], 64, 1), pltpu.roll(x[3], 32, 1)
                r5 = pltpu.roll(x[5], 96, 1)
                tiles += [jnp.where(lane < 96, x[0], r1), jnp.where(lane < 64, r1, r2),
                          jnp.where(lane < 32, r2, r3), jnp.where(lane < 96, x[4], r5)]
                last.append(r5 if cc == 0 else pltpu.roll(x[5], 32, 1))
            tiles.append(jnp.where(lane < 64, last[0], last[1]))
            halves.append(jnp.concatenate([t.astype(jnp.bfloat16) for t in tiles], axis=1))
        out = dot(cc_ref[...], jnp.concatenate(halves, axis=0))
        for cc in range(2):
            dest = dest_chip * 2 + cc
            for t in range(4):
                tile = out[:, (cc * 4 + t) * 128:(cc * 4 + t + 1) * 128].astype(jnp.bfloat16)
                for g in range(12):
                    send[pp, dest, g * 4 + t] = tile[g * 16:(g + 1) * 16]
        low = iota((16, 128), 1) < 64
        for u in range(6):
            upper = out[u * 32:u * 32 + 16, 1024:]
            lower = out[u * 32 + 16:u * 32 + 32, 1024:]
            send[pp, dest_chip * 2, 48 + u] = jnp.where(low, upper, pltpu.roll(lower, 64, 1)).astype(jnp.bfloat16)
            send[pp, dest_chip * 2 + 1, 48 + u] = jnp.where(low, pltpu.roll(upper, 64, 1), lower).astype(jnp.bfloat16)

    def send_groups(pp, groups):
        for group in groups:
            for slot in group:
                pack(pp, slot)

            @pl.loop(0, TILES // PARTS[pp])
            def _(part):
                for cc in range(2):
                    for slot in group:
                        if slot < 7:
                            copy_out(pp, chip_of(slot) * 2 + cc, part).start()
                        elif cc == 1:
                            copy_out(pp, chip * 2 + 1 - core, part).start()

    def copy_own(pp):
        return pltpu.make_async_copy(send.at[pp, me], block(pp, me, pl.ds(0, TILES)), own_sem.at[pp])

    half_transform(0, 0, HEAD, 2)
    row = iota((2 * N, N), 0)
    pick_a = onehot(iota((2 * N, N), 1) == 8 * (row // 16) + row % 8)
    c_rows = dot(pick_a, c, ((1,), (1,))).astype(jnp.bfloat16)
    wide = dot(c_rows, onehot(iota((N, 2 * N), 1) % N == iota((N, 2 * N), 0)))
    same_p = (iota((2 * N, 2 * N), 0) % 16) // 8 == iota((2 * N, 2 * N), 1) // N
    cc_ref[...] = jnp.where(same_p, wide, 0.0).astype(jnp.bfloat16)
    pl.semaphore_wait(barrier, DEV - 1)
    send_groups(0, ((0, 1),))
    half_transform(0, HEAD, N - HEAD, 1, wait=False)
    for idx in range(8):
        load(1, idx).start()
    send_groups(0, FIRST_GROUPS)
    copy_own(0).start()
    for pp in range(1, PAIRS):
        half_transform(pp, 0, N, 1)
        if pp < PAIRS - 1:
            for idx in range(8):
                load(pp + 1, idx).start()
        send_groups(pp, LATER_GROUPS)
        copy_own(pp).start()

    spread = dot(onehot(iota((K8, N), 0) // 8 == iota((K8, N), 1)), c, ((1,), (1,))).astype(jnp.bfloat16)
    col, p_row = iota((N, KP), 1), iota((N, KP), 0)
    same = iota((K8, KP), 0) % 8 == iota((K8, KP), 1) % 8
    for pp in range(PAIRS):
        full = dot(spread, onehot(p_row == (col // 16) * COLS + 2 * pp + (col % 16) // 8))
        kc = jnp.where(same, full, 0.0).astype(jnp.bfloat16)
        if pp < PAIRS - 1:
            kc_first[:, pp * KP:(pp + 1) * KP] = kc
        else:
            kc_ref[...] = kc

    for pp in range(PAIRS - 1):
        copy_own(pp).wait()

        @pl.loop(1, DEV)
        def _(k):
            wait_recv(pp, (me + k) % DEV)

    def rhs_first(tile):
        return jnp.concatenate([g_first[pp, :, tile].reshape(KP, 128) for pp in range(PAIRS - 1)], axis=0)

    for third, vm_ref in enumerate((vm0_ref, vm1_ref, vm2_ref)):
        @pl.loop(0, 4)
        def _(g):
            for n in range(2):
                rhs = jnp.concatenate([rhs_first((4 * third + g) * 4 + 2 * n + t) for t in range(2)], axis=1)
                vm_ref[g, :, n * 256:(n + 1) * 256] = dot(kc_first[...], rhs)

    @pl.loop(0, 6)
    def _(u):
        vh_ref[u] = dot(kc_first[...], rhs_first(48 + u))

    for pp in range(PAIRS):
        @pl.loop(1, DEV)
        def _(k):
            copy_out(pp, (me + k) % DEV).wait_send()

    copy_own(PAIRS - 1).wait()

    @pl.loop(1, DEV)
    def _(k):
        wait_recv(PAIRS - 1, (me + k) % DEV)


def last_kernel(g_ref, vm0_ref, vm1_ref, vm2_ref, vh_ref, kc_ref, v_hbm, slots, sems):
    def put(g, slot):
        rows = pl.ds(pl.multiple_of(8 * g, 8), 8)
        return pltpu.make_async_copy(slots.at[slot], v_hbm.at[:, rows], sems.at[slot])

    for third, vm_ref in enumerate((vm0_ref, vm1_ref, vm2_ref)):
        @pl.loop(0, 2)
        def _(h):
            u = 2 * third + h
            kc = kc_ref[...]
            both = vh_ref[u] + dot(kc, g_ref[:, 48 + u].reshape(KP, 128))
            for parity in range(2):
                slot = 2 * h + parity
                g = 4 * third + slot
                if third > 0:
                    put(g - 4, slot).wait()
                for n in range(2):
                    rhs = jnp.concatenate([g_ref[:, g * 4 + 2 * n + t].reshape(KP, 128) for t in range(2)], axis=1)
                    out = vm_ref[slot, :, n * 256:(n + 1) * 256] + dot(kc, rhs)
                    slots[slot, :, :, n * 256:(n + 1) * 256] = out.reshape(N, 8, 256)
                edge = both if parity == 0 else pltpu.roll(both, 64, 1)
                slots[slot, :, :, 512:576] = edge.reshape(N, 8, 128)[:, :, :64]
                put(g, slot).start()

    for slot in range(4):
        put(8 + slot, slot).wait()


def solution(mesh):
    def local_transform(ao_rows, coeffs):
        vmem = pl.BlockSpec(memory_space=pltpu.VMEM)
        hbm = pl.BlockSpec(memory_space=pltpu.HBM)
        parts = pl.pallas_call(
            exchange_kernel,
            out_shape=(pltpu.VMEM((DEV, TILES, 16, 128), jnp.bfloat16),
                       *[pltpu.VMEM((4, K8, 512), jnp.float32)] * 3,
                       pltpu.VMEM((6, K8, 128), jnp.float32),
                       pltpu.VMEM((K8, KP), jnp.bfloat16)),
            in_specs=[hbm, hbm],
            out_specs=(vmem,) * 6,
            scratch_shapes=[
                pltpu.VMEM((2, N, N, N), jnp.bfloat16),
                pltpu.VMEM((N, N), jnp.bfloat16),
                pltpu.VMEM((N, N), jnp.bfloat16),
                pltpu.VMEM((2, N * QPAD, 128), jnp.float32),
                pltpu.VMEM((PAIRS, DEV, TILES, 16, 128), jnp.bfloat16),
                pltpu.VMEM((PAIRS - 1, DEV, TILES, 16, 128), jnp.bfloat16),
                pltpu.VMEM((2 * N, 2 * N), jnp.bfloat16),
                pltpu.VMEM((K8, (PAIRS - 1) * KP), jnp.bfloat16),
                pltpu.SemaphoreType.DMA((8,)),
                pltpu.SemaphoreType.DMA,
                pltpu.SemaphoreType.DMA((PAIRS, DEV)),
                pltpu.SemaphoreType.DMA((PAIRS, DEV)),
                pltpu.SemaphoreType.DMA((PAIRS,)),
            ],
            compiler_params=pltpu.CompilerParams(collective_id=0, has_side_effects=True, vmem_limit_bytes=34 * 2**20),
            cost_estimate=pl.CostEstimate(flops=10**10, bytes_accessed=40 * 10**6, transcendentals=0),
            name='exchange',
        )(*[pltpu.with_memory_space_constraint(x, pltpu.HBM) for x in (ao_rows, coeffs)])
        return pl.pallas_call(
            last_kernel,
            out_shape=jax.ShapeDtypeStruct((N, N, COLS * N), jnp.float32),
            in_specs=[vmem] * 6,
            out_specs=pl.BlockSpec(memory_space=pltpu.HBM),
            scratch_shapes=[pltpu.VMEM((4, N, 8, COLS * N), jnp.float32), pltpu.SemaphoreType.DMA((4,))],
            compiler_params=pltpu.CompilerParams(vmem_limit_bytes=12 * 2**20),
            cost_estimate=pl.CostEstimate(flops=3 * 10**9, bytes_accessed=24 * 10**6, transcendentals=0),
            name='last_product',
        )(*[pltpu.with_memory_space_constraint(x, pltpu.VMEM) for x in parts])

    return jax.shard_map(local_transform, mesh=mesh, in_specs=(P(('frag', 'dev')), P('frag')), out_specs=P('frag', None, 'dev'), check_vma=False)
```

```python
import jax
import jax.numpy as jnp
from jax import lax
from jax.experimental import pallas as pl
from jax.experimental.pallas import tpu as pltpu
from jax.sharding import PartitionSpec as P

MESH = pl.DeviceIdType.MESH
N = 96
DEV = 16
PAIRS = 3
COLS = 6
QPAD = 104
QB = 24
TILES = 54
PART = 9
K8 = 8 * N
KP = 16 * DEV
HEAD = 32
FIRST_GROUPS = ((2, 3), (4, 5, 6, 7))
LATER_GROUPS = ((0, 3, 4, 6, 1, 2, 5, 7),)


def iota(shape, dim):
    return lax.broadcasted_iota(jnp.int32, shape, dim)


def onehot(mask):
    return jnp.where(mask, 1.0, 0.0).astype(jnp.bfloat16)


def dot(x, y, dims=((1,), (0,))):
    return lax.dot_general(x, y, (dims, ((), ())), preferred_element_type=jnp.float32)


def exchange_kernel(a_hbm, c_hbm, g_last, vm0_ref, vm1_ref, vm2_ref, vh_ref, kc_ref,
                    a_vm, c_vm, ct_ref, h_scr, send, g_first, cc_ref, kc_first, a_sem, c_sem, send_sem, recv_sem, own_sem):
    frag = lax.axis_index('frag')
    me = lax.axis_index('dev')
    chip, core = me // 2, me % 2
    cz1, cz0, cy = chip // 4, (chip // 2) % 2, chip % 2

    def chip_of(slot):
        m = 7 - slot
        return 4 * ((cz1 + m // 4) % 2) + 2 * ((cz0 + (m // 2) % 2) % 2) + (cy + m % 2) % 2

    def load(pp, idx):
        p2, quarter = idx // 4, pl.ds((idx % 4) * QB, QB)
        return pltpu.make_async_copy(a_hbm.at[2 * pp + p2, quarter], a_vm.at[p2, quarter], a_sem.at[idx])

    load_c = pltpu.make_async_copy(c_hbm, c_vm, c_sem)
    load_c.start()
    for idx in range(8):
        load(0, idx).start()

    barrier = pltpu.get_barrier_semaphore()

    @pl.loop(1, DEV)
    def _(k):
        pl.semaphore_signal(barrier, inc=1, device_id=(frag, (me + k) % DEV), device_id_type=MESH)

    load_c.wait()
    c = c_vm[...]
    j_row = iota((N, N), 0)
    pick_j = onehot(iota((N, N), 1) == 2 * COLS * chip_of(j_row // (2 * COLS)) + j_row % (2 * COLS))
    ct_ref[...] = dot(pick_j, c, ((1,), (1,))).astype(jnp.bfloat16)
    stacked = dot(onehot(iota((256, N), 0) % 128 == iota((256, N), 1)), c).astype(jnp.bfloat16)
    both = dot(stacked, onehot(iota((N, 256), 1) % 128 == iota((N, 256), 0)))
    c_two = jnp.where(iota((256, 256), 0) // 128 == iota((256, 256), 1) // 128, both, 0.0).astype(jnp.bfloat16)
    gap = jnp.zeros((N, 32), jnp.bfloat16)
    row = iota((2 * N, N), 0)
    pick_a = onehot(iota((2 * N, N), 1) == 8 * (row // 16) + row % 8)
    c_rows = dot(pick_a, c, ((1,), (1,))).astype(jnp.bfloat16)
    wide = dot(c_rows, onehot(iota((N, 2 * N), 1) % N == iota((N, 2 * N), 0)))
    same_p = (iota((2 * N, 2 * N), 0) % 16) // 8 == iota((2 * N, 2 * N), 1) // N
    cc_ref[...] = jnp.where(same_p, wide, 0.0).astype(jnp.bfloat16)

    lane = iota((N, 128), 1)

    def block(pp, src, tiles):
        if isinstance(pp, int) and pp == PAIRS - 1:
            return g_last.at[src, tiles]
        return g_first.at[pp, src, tiles]

    def copy_out(pp, dest, part=None):
        tiles = pl.ds(0, TILES) if part is None else pl.ds(part * PART, PART)
        return pltpu.make_async_remote_copy(
            src_ref=send.at[pp, dest, tiles],
            dst_ref=block(pp, me, tiles),
            send_sem=send_sem.at[pp, dest],
            recv_sem=recv_sem.at[pp, me],
            device_id=(frag, dest),
            device_id_type=MESH,
        )

    def wait_recv(pp, src):
        tiles = pl.ds(0, TILES)
        pltpu.make_async_remote_copy(
            src_ref=send.at[pp, src, tiles], dst_ref=block(pp, src, tiles),
            send_sem=send_sem.at[pp, src], recv_sem=recv_sem.at[pp, src],
            device_id=(frag, src), device_id_type=MESH,
        ).wait_recv()

    def half_transform(pp, first, rows, loads, wait=True):
        @pl.loop(0, 8 // loads)
        def _(step):
            if wait:
                for i in range(loads):
                    load(pp, step * loads + i).wait()
            p2, q0 = step * loads // 4, (step * loads % 4) * QB
            t_rows = []
            for i in range(0, loads * QB, 2):
                two = jnp.concatenate([a_vm[p2, q0 + i], gap, a_vm[p2, q0 + i + 1], gap], axis=1)
                t_rows.append(dot(ct_ref[first:first + rows], two).astype(jnp.bfloat16))
            half = dot(jnp.concatenate(t_rows, axis=0), c_two)
            for i in range(loads * QB):
                part = half[(i // 2) * rows:(i // 2 + 1) * rows, (i % 2) * 128:(i % 2 + 1) * 128]
                h_scr[p2, pl.ds(first * QPAD + q0 + i, rows, stride=QPAD), :] = part

    def pack(pp, slot):
        dest_chip = chip_of(slot)
        halves = []
        for p in range(2):
            tiles, last = [], []
            for cc in range(2):
                j0 = (slot * 2 + cc) * COLS
                x = [h_scr[p, pl.ds((j0 + l) * QPAD, N), :] for l in range(COLS)]
                r1, r2, r3 = pltpu.roll(x[1], 96, 1), pltpu.roll(x[2], 64, 1), pltpu.roll(x[3], 32, 1)
                r5 = pltpu.roll(x[5], 96, 1)
                tiles += [jnp.where(lane < 96, x[0], r1), jnp.where(lane < 64, r1, r2),
                          jnp.where(lane < 32, r2, r3), jnp.where(lane < 96, x[4], r5)]
                last.append(r5 if cc == 0 else pltpu.roll(x[5], 32, 1))
            tiles.append(jnp.where(lane < 64, last[0], last[1]))
            halves.append(jnp.concatenate([t.astype(jnp.bfloat16) for t in tiles], axis=1))
        out = dot(cc_ref[...], jnp.concatenate(halves, axis=0))
        for cc in range(2):
            dest = dest_chip * 2 + cc
            for t in range(4):
                tile = out[:, (cc * 4 + t) * 128:(cc * 4 + t + 1) * 128].astype(jnp.bfloat16)
                for g in range(12):
                    send[pp, dest, g * 4 + t] = tile[g * 16:(g + 1) * 16]
        low = iota((16, 128), 1) < 64
        for u in range(6):
            upper = out[u * 32:u * 32 + 16, 1024:]
            lower = out[u * 32 + 16:u * 32 + 32, 1024:]
            send[pp, dest_chip * 2, 48 + u] = jnp.where(low, upper, pltpu.roll(lower, 64, 1)).astype(jnp.bfloat16)
            send[pp, dest_chip * 2 + 1, 48 + u] = jnp.where(low, pltpu.roll(upper, 64, 1), lower).astype(jnp.bfloat16)

    def send_groups(pp, groups):
        for group in groups:
            for slot in group:
                pack(pp, slot)

            @pl.loop(0, TILES // PART)
            def _(part):
                for cc in range(2):
                    for slot in group:
                        if slot < 7:
                            copy_out(pp, chip_of(slot) * 2 + cc, part).start()
                        elif cc == 1:
                            copy_out(pp, chip * 2 + 1 - core, part).start()

    def copy_own(pp):
        return pltpu.make_async_copy(send.at[pp, me], block(pp, me, pl.ds(0, TILES)), own_sem.at[pp])

    half_transform(0, 0, HEAD, 2)
    pl.semaphore_wait(barrier, DEV - 1)
    send_groups(0, ((0, 1),))
    half_transform(0, HEAD, N - HEAD, 1, wait=False)
    for idx in range(8):
        load(1, idx).start()
    send_groups(0, FIRST_GROUPS)
    copy_own(0).start()
    for pp in range(1, PAIRS):
        half_transform(pp, 0, N, 1)
        if pp < PAIRS - 1:
            for idx in range(8):
                load(pp + 1, idx).start()
        send_groups(pp, ((0, 1, 2, 3), (4, 5, 6, 7)) if pp == 1 else LATER_GROUPS)
        copy_own(pp).start()

    spread = dot(onehot(iota((K8, N), 0) // 8 == iota((K8, N), 1)), c, ((1,), (1,))).astype(jnp.bfloat16)
    col, p_row = iota((N, KP), 1), iota((N, KP), 0)
    same = iota((K8, KP), 0) % 8 == iota((K8, KP), 1) % 8
    for pp in range(PAIRS):
        full = dot(spread, onehot(p_row == (col // 16) * COLS + 2 * pp + (col % 16) // 8))
        kc = jnp.where(same, full, 0.0).astype(jnp.bfloat16)
        if pp < PAIRS - 1:
            kc_first[:, pp * KP:(pp + 1) * KP] = kc
        else:
            kc_ref[...] = kc

    for pp in range(PAIRS - 1):
        copy_own(pp).wait()

        @pl.loop(1, DEV)
        def _(k):
            wait_recv(pp, (me + k) % DEV)

    def rhs_first(tile):
        return jnp.concatenate([g_first[pp, :, tile].reshape(KP, 128) for pp in range(PAIRS - 1)], axis=0)

    for third, vm_ref in enumerate((vm0_ref, vm1_ref, vm2_ref)):
        @pl.loop(0, 4)
        def _(g):
            for n in range(2):
                rhs = jnp.concatenate([rhs_first((4 * third + g) * 4 + 2 * n + t) for t in range(2)], axis=1)
                vm_ref[g, :, n * 256:(n + 1) * 256] = dot(kc_first[...], rhs)

    @pl.loop(0, 6)
    def _(u):
        vh_ref[u] = dot(kc_first[...], rhs_first(48 + u))

    for pp in range(PAIRS):
        @pl.loop(1, DEV)
        def _(k):
            copy_out(pp, (me + k) % DEV).wait_send()

    copy_own(PAIRS - 1).wait()

    @pl.loop(1, DEV)
    def _(k):
        wait_recv(PAIRS - 1, (me + k) % DEV)


def last_kernel(g_ref, vm0_ref, vm1_ref, vm2_ref, vh_ref, kc_ref, v_hbm, slots, sems):
    def put(g, slot):
        rows = pl.ds(pl.multiple_of(8 * g, 8), 8)
        return pltpu.make_async_copy(slots.at[slot], v_hbm.at[:, rows], sems.at[slot])

    for third, vm_ref in enumerate((vm0_ref, vm1_ref, vm2_ref)):
        @pl.loop(0, 2)
        def _(h):
            u = 2 * third + h
            kc = kc_ref[...]
            both = vh_ref[u] + dot(kc, g_ref[:, 48 + u].reshape(KP, 128))
            for parity in range(2):
                slot = 2 * h + parity
                g = 4 * third + slot
                if third > 0:
                    put(g - 4, slot).wait()
                for n in range(2):
                    rhs = jnp.concatenate([g_ref[:, g * 4 + 2 * n + t].reshape(KP, 128) for t in range(2)], axis=1)
                    out = vm_ref[slot, :, n * 256:(n + 1) * 256] + dot(kc, rhs)
                    slots[slot, :, :, n * 256:(n + 1) * 256] = out.reshape(N, 8, 256)
                edge = both if parity == 0 else pltpu.roll(both, 64, 1)
                slots[slot, :, :, 512:576] = edge.reshape(N, 8, 128)[:, :, :64]
                put(g, slot).start()

    for slot in range(4):
        put(8 + slot, slot).wait()


def solution(mesh):
    def local_transform(ao_rows, coeffs):
        vmem = pl.BlockSpec(memory_space=pltpu.VMEM)
        hbm = pl.BlockSpec(memory_space=pltpu.HBM)
        parts = pl.pallas_call(
            exchange_kernel,
            out_shape=(pltpu.VMEM((DEV, TILES, 16, 128), jnp.bfloat16),
                       *[pltpu.VMEM((4, K8, 512), jnp.float32)] * 3,
                       pltpu.VMEM((6, K8, 128), jnp.float32),
                       pltpu.VMEM((K8, KP), jnp.bfloat16)),
            in_specs=[hbm, hbm],
            out_specs=(vmem,) * 6,
            scratch_shapes=[
                pltpu.VMEM((2, N, N, N), jnp.bfloat16),
                pltpu.VMEM((N, N), jnp.bfloat16),
                pltpu.VMEM((N, N), jnp.bfloat16),
                pltpu.VMEM((2, N * QPAD, 128), jnp.float32),
                pltpu.VMEM((PAIRS, DEV, TILES, 16, 128), jnp.bfloat16),
                pltpu.VMEM((PAIRS - 1, DEV, TILES, 16, 128), jnp.bfloat16),
                pltpu.VMEM((2 * N, 2 * N), jnp.bfloat16),
                pltpu.VMEM((K8, (PAIRS - 1) * KP), jnp.bfloat16),
                pltpu.SemaphoreType.DMA((8,)),
                pltpu.SemaphoreType.DMA,
                pltpu.SemaphoreType.DMA((PAIRS, DEV)),
                pltpu.SemaphoreType.DMA((PAIRS, DEV)),
                pltpu.SemaphoreType.DMA((PAIRS,)),
            ],
            compiler_params=pltpu.CompilerParams(collective_id=0, has_side_effects=True, vmem_limit_bytes=34 * 2**20),
            cost_estimate=pl.CostEstimate(flops=10**10, bytes_accessed=40 * 10**6, transcendentals=0),
            name='exchange',
        )(*[pltpu.with_memory_space_constraint(x, pltpu.HBM) for x in (ao_rows, coeffs)])
        return pl.pallas_call(
            last_kernel,
            out_shape=jax.ShapeDtypeStruct((N, N, COLS * N), jnp.float32),
            in_specs=[vmem] * 6,
            out_specs=pl.BlockSpec(memory_space=pltpu.HBM),
            scratch_shapes=[pltpu.VMEM((4, N, 8, COLS * N), jnp.float32), pltpu.SemaphoreType.DMA((4,))],
            compiler_params=pltpu.CompilerParams(vmem_limit_bytes=12 * 2**20),
            cost_estimate=pl.CostEstimate(flops=3 * 10**9, bytes_accessed=24 * 10**6, transcendentals=0),
            name='last_product',
        )(*[pltpu.with_memory_space_constraint(x, pltpu.VMEM) for x in parts])

    return jax.shard_map(local_transform, mesh=mesh, in_specs=(P(('frag', 'dev')), P('frag')), out_specs=P('frag', None, 'dev'), check_vma=False)
```
